32 devices in a mesh: chip: 8 (over y, x, core), line: 4 (over z).
Axes of the slice: x: 2, y: 2, z: 4, core: 2. Of those that a mesh axis runs over, the one named last changes fastest.
Arguments:
- echoes: bfloat16 [8, 2, 4096, 4096], P('chip', None, 'line'), may hold values from -6 to 6
- range_filter: float32 [2, 4096], replicated, may hold values from -6 to 6
- rcmc_weights: float32 [8, 4096], replicated, may hold values from -3 to 3
- fm_rate: float32 [8, 384], P('chip', 'line'), may hold values from 256 to 2048
- rcmc_shift: int32 [8, 384], P('chip', 'line'), may hold values from 0 to 12, as said below
- seam_width: int32 [8], P('chip'), may hold values from 64 to 128, as said below
- seam_link: int32 [8], P('chip'), may hold values from 0 to 1
Outputs:
- image: bfloat16 [8, 2, 384, 4096], P('chip', None, 'line')
The draws below stay inside these ranges and needn't reach their ends.
Inputs may be any that keep to these rules, and one draw needn't show every extreme that they name: `rcmc_shift`: every draw has some entry equal to 12. `seam_width`: every draw has some chip with the width 128.
All inputs are finite; a program needn't handle non-finite values.
Results may differ from the reference program's by a relative error of at most 0.0011.
Values sent between devices are 32-bit elements; how exact they have to be, the bound alone decides.
No kernel may reach another device: no remote copies, remote signals or barrier semaphores. Data moves between devices by JAX's collectives and lax.ppermute only.
A program may use at most 192 MiB of HBM per device.

```python
import math
import jax
import jax.numpy as jnp
from jax import lax

AZ = 4096
RG = 4096
RKEEP = 384
TAPS = 8
MAXSHIFT = 12
OVL = 128
CHIPS = 8


def draw_rcmc_shift(key, part):
    first, second = jax.random.split(jax.random.fold_in(key, 11))
    values = jax.random.randint(first, (CHIPS, RKEEP), 0, MAXSHIFT + 1, dtype=jnp.int32)
    where_max = jax.random.randint(second, (), 0, CHIPS * RKEEP, dtype=jnp.int32)
    flattened = values.reshape(-1).at[where_max].set(MAXSHIFT)
    return flattened.reshape(CHIPS, RKEEP)


def draw_seam_width(key, part):
    first, second = jax.random.split(jax.random.fold_in(key, 23))
    values = jax.random.randint(first, (CHIPS,), OVL // 2, OVL + 1, dtype=jnp.int32)
    where_max = jax.random.randint(second, (), 0, CHIPS, dtype=jnp.int32)
    return values.at[where_max].set(OVL)


def draw_seam_link(key, part):
    values = jax.random.randint(jax.random.fold_in(key, 37), (CHIPS,), 0, 4, dtype=jnp.int32)
    linked = (values > 0).astype(jnp.int32)
    return linked.at[0].set(0)


def shard_levels(rng, shape, pieces, smallest, high):
    factor_of, own = 1.0, jax.random.fold_in(rng, 6)
    for axis_at, shards_of in pieces:
        steps = jnp.exp(jax.random.uniform(jax.random.fold_in(own, axis_at), (shards_of,), jnp.float32, smallest / len(pieces), high / len(pieces)))
        factor_of = factor_of * jnp.repeat(steps, shape[axis_at] // shards_of).reshape([-1 if axis == axis_at else 1 for axis in range(len(shape))])
    return factor_of


def noise(own_key, extent, deviation, reach, pieces=(), kind=jnp.bfloat16):
    level = shard_levels(own_key, extent, pieces, -0.22, 0.18) if pieces else 1.0
    entries = jax.random.normal(own_key, extent, jnp.float32) * deviation * level
    return jnp.minimum(jnp.maximum(entries, -reach), reach).astype(kind)


def setup_inputs(seed: int = 0) -> dict:
    key_list = jax.random.split(jax.random.key(seed), 8)
    echoes = noise(key_list[0], (CHIPS, 2, AZ, RG), 1.0, 6.0, ((0, 8), (2, 4)))
    range_filter = noise(key_list[1], (2, RG), 1.0, 6.0, (), jnp.float32)
    rcmc_weights = noise(key_list[2], (TAPS, AZ), 0.5, 3.0, (), jnp.float32)
    fm_rate = jnp.clip(jnp.exp(math.log(2048.0) - 2.0794415 * jax.random.uniform(key_list[3], (CHIPS, RKEEP), jnp.float32) ** shard_levels(key_list[3], (CHIPS, RKEEP), ((0, 8), (1, 4)), -0.2, 0.2)), 256.0, 2048.0)
    rcmc_shift = draw_rcmc_shift(jax.random.fold_in(key_list[7], 71), 0)
    seam_width = draw_seam_width(jax.random.fold_in(key_list[7], 71), 0)
    seam_link = draw_seam_link(jax.random.fold_in(key_list[7], 71), 0)
    return {"echoes": echoes, "range_filter": range_filter, "rcmc_weights": rcmc_weights, "fm_rate": fm_rate, "rcmc_shift": rcmc_shift, "seam_width": seam_width, "seam_link": seam_link}


def reference(echoes, range_filter, rcmc_weights, fm_rate, rcmc_shift, seam_width, seam_link):
    margin = MAXSHIFT + TAPS - 1
    filter_pair = lax.complex(range_filter[0], range_filter[1])

    def focus_chip(inputs):
        echo, rate, shift = inputs
        raw = lax.complex(echo[0].astype(jnp.float32), echo[1].astype(jnp.float32))
        compressed = jnp.fft.ifft(jnp.fft.fft(raw, axis=1) * filter_pair[None], axis=1)[:, :RKEEP]
        gain = 1.0 + 2.0 * jnp.arange(RKEEP, dtype=jnp.float32) / RKEEP
        compressed = compressed * gain[None]
        doppler = jnp.fft.fft(compressed, axis=0).T
        padded = jnp.concatenate([doppler, jnp.zeros((margin, AZ), doppler.dtype)], axis=0)
        positions = jnp.arange(RKEEP, dtype=jnp.int32) + shift
        migrated = jnp.zeros((RKEEP, AZ), doppler.dtype)
        for offset in range(TAPS):
            migrated = migrated + rcmc_weights[offset][None] * jnp.take(padded, positions + offset, axis=0)
        index = jnp.arange(AZ, dtype=jnp.int32)
        frequency = ((index + AZ // 2) % AZ - AZ // 2).astype(jnp.float32) / AZ
        phase = math.pi * (rate[:, None] * (frequency * frequency)[None, :])
        filtered = migrated * lax.complex(jnp.cos(phase), -jnp.sin(phase))
        focused = jnp.fft.ifft(filtered, axis=1)
        return jnp.stack([jnp.real(focused), jnp.imag(focused)])
    focused = lax.map(focus_chip, (echoes, fm_rate, rcmc_shift))
    tails = jnp.concatenate([jnp.zeros((1, 2, RKEEP, OVL), focused.dtype), focused[:-1, :, :, AZ - OVL:]], axis=0)
    offsets = jnp.arange(OVL, dtype=jnp.int32)
    columns = jnp.clip(OVL - seam_width[:, None] + offsets[None], 0, OVL - 1)
    previous = jax.vmap(lambda tail_block, column: jnp.take(tail_block, column, axis=2))(tails, columns)
    ramp = (offsets.astype(jnp.float32)[None] + 0.5) / seam_width[:, None].astype(jnp.float32)
    inside = (offsets[None] < seam_width[:, None]) & (seam_link[:, None] == 1)
    ramp = ramp[:, None, None, :]
    inside = inside[:, None, None, :]
    head = focused[:, :, :, :OVL]
    mixed = jnp.where(inside, (1.0 - ramp) * previous + ramp * head, head)
    blended = jnp.concatenate([mixed, focused[:, :, :, OVL:]], axis=3)
    energy = lax.optimization_barrier(jnp.sum(blended * blended, axis=(1, 2, 3)))
    scale = lax.rsqrt(energy / (RKEEP * AZ) + 1e-06)
    return (blended * scale[:, None, None, None]).astype(jnp.bfloat16)
```

```python
import math

import jax
import jax.numpy as jnp
import numpy as np
from jax import lax
from jax.experimental import pallas as pl
from jax.experimental.pallas import tpu as pltpu
from jax.sharding import PartitionSpec as P


RKEEP = 384
TAPS = 8
MAXSHIFT = 12
LANES = 128
MARGIN = MAXSHIFT + TAPS - 1

F32 = jnp.float32
ANY = pl.BlockSpec(memory_space=pl.ANY)
VMEM = pl.BlockSpec(memory_space=pltpu.VMEM)
BF16 = jnp.bfloat16


def split_np(table):
    high = table.astype(jnp.bfloat16)
    low = (table - high.astype(np.float64)).astype(jnp.bfloat16)
    return high, low


def root(length, index, sign):
    angle = sign * 2.0 * np.pi * (np.asarray(index) % length) / length
    return np.cos(angle), np.sin(angle)


def lane_matrix(sign, scale=1.0):
    index = np.arange(LANES)
    real, imag = root(LANES, np.outer(index, index), sign)
    full = scale * np.block([[real, imag], [-imag, real]])
    high, low = split_np(full)
    return np.concatenate([high, high, low], axis=0)


def column_twiddle(columns, length, sign, scale=1.0):
    real, imag = root(length, np.outer(np.arange(columns), np.arange(LANES)), sign)
    return (scale * np.stack([real, imag])).astype(np.float32)


def cmul_const(value, real, imag):
    vr, vi = value
    near = 1e-12
    if abs(imag) < near:
        if abs(real - 1.0) < near:
            return value
        if abs(real + 1.0) < near:
            return (-vr, -vi)
    if abs(real) < near:
        if imag > 0:
            return (-vi, vr)
        return (vi, -vr)
    if abs(abs(real) - abs(imag)) < near:
        mag = abs(real)
        sr, si = (1.0 if real > 0 else -1.0), (1.0 if imag > 0 else -1.0)
        if sr == si:
            return ((vr - vi) * (mag * sr), (vr + vi) * (mag * sr))
        return ((vr + vi) * (mag * sr), (vi - vr) * (mag * sr))
    return (vr * real - vi * imag, vr * imag + vi * real)


def cadd(a, b):
    return (a[0] + b[0], a[1] + b[1])


def csub(a, b):
    return (a[0] - b[0], a[1] - b[1])


def dft_list(values, sign):
    count = len(values)
    if count == 1:
        return values
    if count == 2:
        return [cadd(values[0], values[1]), csub(values[0], values[1])]
    if count == 4:
        even = [cadd(values[0], values[2]), csub(values[0], values[2])]
        odd = [cadd(values[1], values[3]), csub(values[1], values[3])]
        turn = cmul_const(odd[1], 0.0, float(sign))
        return [cadd(even[0], odd[0]), cadd(even[1], turn), csub(even[0], odd[0]), csub(even[1], turn)]
    even = dft_list(values[0::2], sign)
    odd = dft_list(values[1::2], sign)
    low, high = [], []
    for k in range(count // 2):
        real, imag = root(count, k, sign)
        turned = cmul_const(odd[k], float(real), float(imag))
        low.append(cadd(even[k], turned))
        high.append(csub(even[k], turned))
    return low + high


def split3(value):
    high = value.astype(BF16)
    low = (value - high.astype(F32)).astype(BF16)
    return high, low


def dot_nn(a, b):
    return lax.dot_general(a, b, (((1,), (0,)), ((), ())), preferred_element_type=F32)


def dot_nt(a, b):
    return lax.dot_general(a, b, (((1,), (1,)), ((), ())), preferred_element_type=F32)


def response_tables(length):
    columns = length // LANES
    group = LANES // columns
    index = np.arange(LANES)
    firsts = []
    for b in range(group):
        real, imag = root(LANES, np.outer(index, np.arange(columns) * group + b), -1)
        firsts.append(np.block([[real, -imag], [imag, real]]))
    first = np.concatenate(firsts, axis=1).astype(np.float32)
    tw = column_twiddle(columns, length, -1, 1.0 / length).reshape(2 * columns, LANES)
    real, imag = root(columns, np.outer(np.arange(columns), np.arange(columns)), -1)
    last = np.block([[real, -imag], [imag, real]]).astype(np.float32)
    table = np.zeros((2 * LANES + 2 * columns, max(2 * LANES, LANES + 2 * columns)), np.float32)
    table[:2 * LANES, :2 * LANES] = first
    table[2 * LANES:, :LANES] = tw
    table[2 * LANES:, LANES:LANES + 2 * columns] = last
    return table


def response(f_ref, table_ref, out_ref):
    columns = out_ref.shape[1]
    group = LANES // columns
    parts = []
    for c in range(2):
        parts.append(jnp.concatenate(
            [f_ref[c:c + 1, j * LANES:(j + 1) * LANES] for j in range(columns)], axis=0))
    blocks = []
    for b in range(group):
        sl = slice(columns * b, columns * (b + 1))
        blocks.append(jnp.concatenate([parts[0][:, sl], parts[1][:, sl]], axis=0))
    rhs = jnp.concatenate(blocks, axis=0)
    half = lax.dot_general(
        table_ref[:2 * LANES, :2 * LANES], rhs, (((1,), (0,)), ((), ())),
        precision=lax.Precision.HIGHEST, preferred_element_type=F32)
    re = half[:LANES].T
    im = half[LANES:].T
    twr = table_ref[2 * LANES:2 * LANES + columns, :LANES]
    twi = table_ref[2 * LANES + columns:2 * LANES + 2 * columns, :LANES]
    pair = jnp.concatenate([re * twr - im * twi, re * twi + im * twr], axis=0)
    full = lax.dot_general(
        table_ref[2 * LANES:, LANES:LANES + 2 * columns], pair, (((1,), (0,)), ((), ())),
        precision=lax.Precision.HIGHEST, preferred_element_type=F32)
    out_ref[0] = full[:columns]
    out_ref[1] = full[columns:]


def toeplitz(g_ref, table, count, per, start, rows, columns):
    base = [
        jnp.concatenate([jnp.broadcast_to(g_ref[c, j:j + 1, :], (8, LANES)) for j in range(columns)], axis=1)
        for c in range(2)
    ]
    base = [pltpu.roll(b, 0, 1, stride=1, stride_axis=0) for b in base]
    sub = lax.broadcasted_iota(jnp.int32, (8, LANES), 0)
    half = count * rows
    group = 16 if half % 16 == 0 else 8
    order = [per * d + start + r8 for d in range(count) for r8 in range(0, rows, 8)]
    for at in range(0, half, group):
        pieces = [[], []]
        for shift in order[at // 8:(at + group) // 8]:
            bins = (sub + shift).astype(F32)
            gain = 1.0 + 2.0 * bins / RKEEP
            gain = jnp.concatenate([gain] * columns, axis=1)
            for c in range(2):
                pieces[c].append(pltpu.roll(base[c], shift % (columns * LANES), 1) * gain)
        grh, grl = split3(jnp.concatenate(pieces[0], axis=0))
        gih, gil = split3(jnp.concatenate(pieces[1], axis=0))
        for n, (plain, crossed) in enumerate(((grh, -gih), (gih, grh), (grl, -gil), (gil, grl))):
            table[0, n * half + at:n * half + at + group, :] = plain
            table[1, n * half + at:n * half + at + group, :] = crossed


def scatter(me_ref, outs, turned):
    count = len(outs)
    for s in range(count):
        dest = lax.rem(me_ref[0] + s, count)
        outs[s][0] = turned[0, dest]
        outs[s][1] = turned[1, dest]


def turn(acc, turned, at):
    width = acc.shape[1] // 2
    both = acc[:, :width] + acc[:, width:]
    turned[:, :, :, pl.ds(at, acc.shape[0])] = both.T.reshape(turned.shape[:3] + (acc.shape[0],))


def compress_first(echoes, range_filter, me, count, per, rows):
    lines, samples = echoes.shape[2], echoes.shape[3]
    columns = samples // LANES
    blocks = max(1, min(4, samples // 1024))
    kblk = samples // blocks
    width = 2 * count * rows
    mblk = min(512, lines)
    tables = response_tables(samples)

    def kernel(me_ref, x_hbm, f_hbm, t_hbm, *refs):
        outs, refs = refs[:count], refs[count:]
        g_ref, x_ref, f_ref, t_ref, table, acc, turned, sems = refs
        small = [pltpu.make_async_copy(f_hbm, f_ref, sems.at[2 * blocks]),
                 pltpu.make_async_copy(t_hbm, t_ref, sems.at[2 * blocks + 1])]
        large = []
        for k in range(blocks):
            for c in range(2):
                ks = slice(k * kblk, (k + 1) * kblk)
                large.append(pltpu.make_async_copy(
                    x_hbm.at[0, c, :, ks], x_ref.at[c, :, ks], sems.at[2 * k + c]))
        for copy in small + large:
            copy.start()
        for copy in small:
            copy.wait()
        response(f_ref, t_ref, g_ref)
        toeplitz(g_ref, table, count, per, 0, rows, columns)
        for k in range(blocks):
            ks = slice(k * kblk, (k + 1) * kblk)
            large[2 * k].wait()
            large[2 * k + 1].wait()

            def body(m, carry):
                at = pl.multiple_of(m * mblk, mblk)
                ms = pl.ds(at, mblk)
                part = dot_nt(x_ref[0, ms, ks], table[0, :, ks]) + dot_nt(x_ref[1, ms, ks], table[1, :, ks])
                if k > 0:
                    part = part + acc[ms, :]
                if k < blocks - 1:
                    acc[ms, :] = part
                else:
                    turn(part, turned, at)
                return carry

            lax.fori_loop(0, lines // mblk, body, 0)
        scatter(me_ref, outs, turned)

    hbm = pl.BlockSpec(memory_space=pltpu.HBM)
    out = jax.ShapeDtypeStruct((2, rows, lines), F32)
    results = pl.pallas_call(
        kernel,
        in_specs=[pl.BlockSpec(memory_space=pltpu.SMEM), hbm, hbm, hbm],
        out_specs=[VMEM] * (count + 2),
        out_shape=[out] * count + [
            jax.ShapeDtypeStruct((2, columns, LANES), F32),
            jax.ShapeDtypeStruct((2, lines, samples), BF16)],
        scratch_shapes=[
            pltpu.VMEM(range_filter.shape, F32),
            pltpu.VMEM(tables.shape, F32),
            pltpu.VMEM((2, 2 * width, samples), BF16),
            pltpu.VMEM((lines, 2 * width), F32),
            pltpu.VMEM((2, count, rows, lines), F32),
            pltpu.SemaphoreType.DMA((2 * blocks + 2,)),
        ],
        compiler_params=pltpu.CompilerParams(vmem_limit_bytes=(26 if rows * count <= 64 else 48) * 2**20),
        cost_estimate=pl.CostEstimate(
            flops=8 * lines * samples * 2 * width, bytes_accessed=4 * lines * samples, transcendentals=0),
        name="compress",
    )(me, echoes, range_filter, tables)
    return results[:count], results[count], results[count + 1]


def compress(x, g, me, count, per, start, rows, after):
    lines, samples = x.shape[1], x.shape[2]
    columns = samples // LANES
    width = 2 * count * rows
    mblk = min(256, lines)

    def kernel(me_ref, x_ref, g_ref, _, *refs):
        outs = refs[:count]
        table, turned = refs[count:]
        toeplitz(g_ref, table, count, per, start, rows, columns)

        def body(m, carry):
            at = pl.multiple_of(m * mblk, mblk)
            ms = pl.ds(at, mblk)
            turn(dot_nt(x_ref[0, ms, :], table[0]) + dot_nt(x_ref[1, ms, :], table[1]), turned, at)
            return carry

        lax.fori_loop(0, lines // mblk, body, 0)
        scatter(me_ref, outs, turned)

    return pl.pallas_call(
        kernel,
        in_specs=[pl.BlockSpec(memory_space=pltpu.SMEM), VMEM, VMEM, ANY],
        out_specs=[VMEM] * count,
        out_shape=[jax.ShapeDtypeStruct((2, rows, lines), F32)] * count,
        scratch_shapes=[
            pltpu.VMEM((2, 2 * width, samples), BF16),
            pltpu.VMEM((2, count, rows, lines), F32),
        ],
        compiler_params=pltpu.CompilerParams(vmem_limit_bytes=(6 + rows * count // 10) * 2**20),
        cost_estimate=pl.CostEstimate(
            flops=8 * lines * samples * 2 * width, bytes_accessed=4 * lines * samples, transcendentals=0),
        name="compress",
    )(me, x, g, after)


def doppler(chunks, tw, matrix, lead, after):
    count = len(chunks[0])
    lines = chunks[0][0].shape[2]
    sizes = [pieces[0].shape[1] for pieces in chunks]
    rows = sum(sizes)
    own = lines // LANES
    columns = own * count
    number = count * len(chunks)

    def kernel(*refs):
        tw_ref, mat_ref = refs[number:number + 2]
        outs, scratch = refs[number + 2 + len(after):-1], refs[-1]
        out_ref = outs[0]
        begun = 0
        for n, size in enumerate(sizes):
            ins = refs[n * count:(n + 1) * count]
            for r8 in range(0, size, 8):
                rs = slice(r8, r8 + 8)
                inner = [[None] * own for _ in range(count)]
                for p in range(own):
                    ls = slice(p * LANES, (p + 1) * LANES)
                    spread = dft_list([(ref[0, rs, ls], ref[1, rs, ls]) for ref in ins], 1)
                    for k0 in range(count):
                        real, imag = root(columns, p * k0, -1)
                        inner[k0][p] = cmul_const(spread[k0], float(real), float(imag))
                for k0 in range(count):
                    for k1, (vr, vi) in enumerate(dft_list(inner[k0], -1)):
                        k = k0 + count * k1
                        tr = tw_ref[0, k:k + 1, :]
                        ti = tw_ref[1, k:k + 1, :]
                        at = k * rows + begun + r8
                        scratch[at:at + 8, :LANES] = vr * tr - vi * ti
                        scratch[at:at + 8, LANES:] = vr * ti + vi * tr
            begun += size
        high, low = split3(scratch[...])
        out = dot_nn(jnp.concatenate([high, low, high], axis=1), mat_ref[...])
        out_ref[0] = out[:, :LANES].reshape(columns, rows, LANES)
        out_ref[1] = out[:, LANES:].reshape(columns, rows, LANES)
        if lead:
            for c in range(2):
                for k in range(columns):
                    at = (c * columns + k) * lead
                    outs[1][at:at + lead, :] = out_ref[c, k, :lead, :]

    return pl.pallas_call(
        kernel,
        in_specs=[VMEM] * (number + 2) + [ANY] * len(after),
        out_shape=[jax.ShapeDtypeStruct((2, columns, rows, LANES), F32)]
        + ([jax.ShapeDtypeStruct((2 * columns * lead, LANES), F32)] if lead else []),
        compiler_params=pltpu.CompilerParams(vmem_limit_bytes=16 * 2**20),
        scratch_shapes=[pltpu.VMEM((columns * rows, 2 * LANES), F32)],
        cost_estimate=pl.CostEstimate(
            flops=2 * columns * rows * 256 * 768, bytes_accessed=16 * columns * rows * LANES, transcendentals=0),
        name="doppler",
    )(*[piece for pieces in chunks for piece in pieces], tw, matrix, *after)


def turn_pair(turns):
    folds = jnp.floor(2.0 * turns + 0.5)
    rest = turns - 0.5 * folds
    sign = 1.0 - 2.0 * (folds - 2.0 * jnp.floor(0.5 * folds))
    z = rest * rest
    cos_c = [(-1) ** j * (2 * math.pi) ** (2 * j) / math.factorial(2 * j) for j in range(7)]
    sin_c = [(-1) ** j * (2 * math.pi) ** (2 * j + 1) / math.factorial(2 * j + 1) for j in range(7)]
    c = cos_c[-1] * z + cos_c[-2]
    s = sin_c[-1] * z + sin_c[-2]
    for j in range(4, -1, -1):
        c = c * z + cos_c[j]
        s = s * z + sin_c[j]
    return c * sign, s * (rest * sign)


def phases(fm, weights, columns, splits):
    pick = np.zeros((LANES, LANES), np.float32)
    width = LANES // columns
    for b in range(width):
        for p in range(columns):
            pick[b * columns + p, width * p + b] = 1.0
    per = fm.shape[0]
    length = columns * LANES
    coarse = 2048
    together = 8

    def kernel(fm_ref, w_ref, pick_ref, *outs):
        outs, w_out = outs[:-1], outs[-1]

        @pl.when(pl.program_id(0) == 0)
        def _():
            rows_in = []
            for t in range(TAPS):
                tap = jnp.concatenate(
                    [w_ref[t:t + 1, p * LANES:(p + 1) * LANES] for p in range(columns)], axis=0).T
                rows_in.append(jnp.concatenate(
                    [tap[b * columns:(b + 1) * columns, :] for b in range(width)], axis=1))
            w_out[...] = lax.dot_general(
                jnp.concatenate(rows_in, axis=0), pick_ref[...], (((1,), (0,)), ((), ())),
                precision=lax.Precision.HIGHEST, preferred_element_type=F32)

        for i in range(together):
            k = pl.program_id(0) * together + i
            lane = lax.broadcasted_iota(jnp.int32, (1, LANES), 1)
            index = k + columns * lane
            index = jnp.where(index >= length // 2, index - length, index)
            square = index * index
            upper = (square // coarse).astype(F32)
            lower = (square % coarse).astype(F32)
            scale = 1.0 / (2.0 * length * length)
            first = 0
            for out, rows in zip(outs, splits):
                rate = fm_ref[first:first + rows, :]
                whole = jnp.floor(rate)
                part = rate - whole
                turns = whole * (upper * (coarse * scale))
                turns = turns - jnp.floor(turns)
                turns = turns + whole * (lower * scale) + part * (square.astype(F32) * scale)
                c, s = turn_pair(turns)
                out[0, i] = c
                out[1, i] = -s
                first += rows

    return pl.pallas_call(
        kernel,
        grid=(columns // together,),
        in_specs=[pl.BlockSpec(a, lambda k: (0, 0)) for a in ((per, LANES), weights.shape, pick.shape)],
        out_specs=[pl.BlockSpec((2, together, rows, LANES), lambda k: (0, k, 0, 0)) for rows in splits]
        + [pl.BlockSpec((TAPS * columns, LANES), lambda k: (0, 0))],
        out_shape=[jax.ShapeDtypeStruct((2, columns, rows, LANES), F32) for rows in splits]
        + [jax.ShapeDtypeStruct((TAPS * columns, LANES), F32)],
        cost_estimate=pl.CostEstimate(
            flops=60 * columns * per * LANES, bytes_accessed=8 * columns * per * LANES, transcendentals=0),
        compiler_params=pltpu.CompilerParams(vmem_limit_bytes=8 * 2**20),
        name="phases",
    )(jnp.broadcast_to(fm[:, None], (per, LANES)), weights, pick)


def focus_rows(parts, weights, shift, phase, tw, matrix, first, rows, earlier):
    columns = phase.shape[1]
    total = sum(take for _, _, take in parts)
    reach = -(-(rows + MAXSHIFT) // 8) * 8
    pitch_d = max(total, reach + 8)
    pitch_d += 1 - pitch_d % 2
    pitch_u = reach + 1
    pitch_m = rows + 1

    def kernel(shift_ref, *refs):
        ins = refs[:len(parts)]
        w_ref, ph_ref, tw_ref, mat_ref = refs[len(parts):len(parts) + 4]
        before = refs[len(parts) + 4:len(parts) + 4 + len(earlier)]
        out_ref, head_ref, tail_ref, en_ref, dop, sums, moved, scratch = refs[len(parts) + 4 + len(earlier):]
        base = 0
        for ref in before:
            tail_ref[:, base:base + ref.shape[1], :] = ref[...]
            base += ref.shape[1]

        def combine(k, carry):
            taps = [w_ref[pl.ds(t * columns + k, 1), :] for t in range(TAPS)]
            for c in range(2):
                at = (c * columns + k) * pitch_d
                filled = 0
                for ref, (a, begin, take) in zip(ins, parts):
                    if len(a.shape) == 4:
                        piece = ref[c, k, begin:begin + take, :]
                    else:
                        piece = ref[pl.ds((c * columns + k) * take, take), :]
                    dop[pl.ds(at + filled, take), :] = piece
                    filled += take
                if filled < reach + 8:
                    dop[pl.ds(at + filled, reach + 8 - filled), :] = jnp.zeros((reach + 8 - filled, LANES), F32)
                to = (c * columns + k) * pitch_u
                for r8 in range(0, reach, 8):
                    value = taps[0] * dop[pl.ds(at + r8, 8), :]
                    for t in range(1, TAPS):
                        value = value + taps[t] * dop[pl.ds(at + r8 + t, 8), :]
                    sums[pl.ds(to + r8, 8), :] = value
            return carry

        lax.fori_loop(0, columns, combine, 0)

        def move(r, carry):
            source = r + shift_ref[first + r]
            for c in range(2):
                for k8 in range(0, columns, 8):
                    lead = c * columns + k8
                    moved[pl.ds(lead * pitch_m + r, 8, stride=pitch_m), :] = (
                        sums[pl.ds(lead * pitch_u + source, 8, stride=pitch_u), :])
            return carry

        lax.fori_loop(0, rows, move, 0)

        for k in range(columns):
            at = slice(k * rows, (k + 1) * rows)
            vr = moved[k * pitch_m:k * pitch_m + rows, :]
            vi = moved[(columns + k) * pitch_m:(columns + k) * pitch_m + rows, :]
            pr, pi = ph_ref[0, k], ph_ref[1, k]
            scratch[at, :LANES] = vr * pr - vi * pi
            scratch[at, LANES:] = vr * pi + vi * pr
        high, low = split3(scratch[...])
        scratch[...] = dot_nn(jnp.concatenate([high, low, high], axis=1), mat_ref[...])
        total_energy = jnp.zeros((8, LANES), F32)
        for r8 in range(0, rows, 8):
            values = []
            for k in range(columns):
                at = slice(k * rows + r8, k * rows + r8 + 8)
                vr, vi = scratch[at, :LANES], scratch[at, LANES:]
                tr, ti = tw_ref[0, k:k + 1, :], tw_ref[1, k:k + 1, :]
                values.append((vr * tr - vi * ti, vr * ti + vi * tr))
            for j, (vr, vi) in enumerate(dft_list(values, 1)):
                ls = slice(j * LANES, (j + 1) * LANES)
                if j == 0:
                    head_ref[0, r8:r8 + 8, :] = vr
                    head_ref[1, r8:r8 + 8, :] = vi
                else:
                    out_ref[0, r8:r8 + 8, ls] = vr
                    out_ref[1, r8:r8 + 8, ls] = vi
                if j == columns - 1:
                    tail_ref[0, base + r8:base + r8 + 8, :] = vr
                    tail_ref[1, base + r8:base + r8 + 8, :] = vi
                if j > 0:
                    total_energy = total_energy + vr * vr + vi * vi
        en_ref[...] = total_energy

    return pl.pallas_call(
        kernel,
        in_specs=[pl.BlockSpec(memory_space=pltpu.SMEM)] + [VMEM] * (len(parts) + 4 + len(earlier)),
        out_shape=[
            jax.ShapeDtypeStruct((2, rows, columns * LANES), F32),
            jax.ShapeDtypeStruct((2, rows, LANES), F32),
            jax.ShapeDtypeStruct((2, rows + sum(a.shape[1] for a in earlier), LANES), F32),
            jax.ShapeDtypeStruct((8, LANES), F32),
        ],
        scratch_shapes=[
            pltpu.VMEM((-(-2 * columns * pitch_d // 8) * 8 + 8, LANES), F32),
            pltpu.VMEM((-(-2 * columns * pitch_u // 8) * 8 + 8, LANES), F32),
            pltpu.VMEM((-(-2 * columns * pitch_m // 8) * 8 + 8, LANES), F32),
            pltpu.VMEM((columns * rows, 2 * LANES), F32),
        ],
        compiler_params=pltpu.CompilerParams(vmem_limit_bytes=(16 if rows < 32 else 30) * 2**20),
        cost_estimate=pl.CostEstimate(
            flops=2 * columns * rows * 256 * 768, bytes_accessed=32 * columns * rows * LANES, transcendentals=0),
        name="focus",
    )(shift, *[a for a, _, _ in parts], weights, phase, tw, matrix, *earlier)


def blend(heads, earlier, energies, seam):
    number = len(heads)

    def kernel(seam_ref, *refs):
        head_refs, tail_ref, energy_refs = refs[:number], refs[number], refs[number + 1:-number - 1]
        outs, total_ref = refs[-number - 1:-1], refs[-1]
        width, linked = seam_ref[0], seam_ref[1]
        total = energy_refs[0][...]
        for ref in energy_refs[1:]:
            total = total + ref[...]
        first = 0
        for head, out in zip(head_refs, outs):
            rows = head.shape[1]
            for c in range(2):
                now = head[c]
                offsets = lax.broadcasted_iota(jnp.int32, now.shape, 1)
                ramp = (offsets.astype(F32) + 0.5) / width.astype(F32)
                inside = (offsets < width) & (linked == 1)
                before = pltpu.roll(tail_ref[c, first:first + rows, :], width, 1)
                mixed = jnp.where(inside, (1.0 - ramp) * before + ramp * now, now)
                out[c] = mixed
                power = mixed * mixed
                for r8 in range(0, rows, 8):
                    total = total + power[r8:r8 + 8]
            first += rows
        total_ref[...] = total

    return pl.pallas_call(
        kernel,
        in_specs=[pl.BlockSpec(memory_space=pltpu.SMEM)] + [VMEM] * (number + 1 + len(energies)),
        out_shape=[jax.ShapeDtypeStruct(h.shape, F32) for h in heads] + [jax.ShapeDtypeStruct((8, LANES), F32)],
        compiler_params=pltpu.CompilerParams(vmem_limit_bytes=4 * 2**20),
        name="blend",
    )(seam, *heads, earlier, *energies)


def finish(images, heads, energies, pixels):
    number, count = len(images), len(energies)
    total_rows = sum(a.shape[1] for a in images)
    length = images[0].shape[2]

    def kernel(*refs):
        image_refs, head_refs = refs[:number], refs[number:2 * number]
        energy_refs, out_ref = refs[2 * number:-1], refs[-1]
        total = energy_refs[0][...]
        for ref in energy_refs[1:]:
            total = total + ref[...]
        energy = jnp.sum(jnp.sum(total, axis=0, keepdims=True), axis=1, keepdims=True)
        scale = lax.rsqrt(energy / pixels + 1e-06)
        for c in range(2):
            for j in range(length // LANES):
                ls = slice(j * LANES, (j + 1) * LANES)
                rows = [ref[c] if j == 0 else ref[c, :, ls] for ref in (head_refs if j == 0 else image_refs)]
                out_ref[0, c, :, ls] = (jnp.concatenate(rows, axis=0) * scale).astype(BF16)

    return pl.pallas_call(
        kernel,
        in_specs=[VMEM] * (2 * number + count),
        out_shape=jax.ShapeDtypeStruct((1, 2, total_rows, length), BF16),
        compiler_params=pltpu.CompilerParams(vmem_limit_bytes=12 * 2**20),
        name="finish",
    )(*images, *heads, *energies)


def cyclic(value, axis, steps):
    count = lax.axis_size(axis)
    return lax.ppermute(value, axis, [(i, (i + steps) % count) for i in range(count)])


def plan(per):
    if per == 96:
        return [16, 32, 48], [[0, 1], [2]], [24, 48, 24]
    return [per], [[0]], [per]


def strip(echoes, range_filter, rcmc_weights, fm_rate, rcmc_shift, seam_width, seam_link):
    count = lax.axis_size("line")
    chips = lax.axis_size("chip")
    me = lax.axis_index("line").astype(jnp.int32)
    lines = echoes.shape[2]
    length = lines * count
    columns = length // LANES
    per = fm_rate.shape[1]

    turn = root(count, np.outer(np.arange(count), np.arange(columns)), -1)
    base = column_twiddle(columns, length, -1).astype(np.float64)
    tw_all = np.stack([
        turn[0][:, :, None] * base[0] - turn[1][:, :, None] * base[1],
        turn[0][:, :, None] * base[1] + turn[1][:, :, None] * base[0]], axis=1).astype(np.float32)
    tw_forward = lax.dynamic_index_in_dim(jnp.asarray(tw_all), me, 0, keepdims=False)
    tw_inverse = column_twiddle(columns, length, 1, 1.0 / length)
    mat_forward = lane_matrix(-1)
    mat_inverse = lane_matrix(1)

    me1 = me.reshape(1)
    sizes, groups, splits = plan(per)
    starts = [sum(sizes[:c]) for c in range(len(sizes))]
    chunks = []
    for c, (begin, rows) in enumerate(zip(starts, sizes)):
        if c == 0:
            outs, g, x = compress_first(echoes, range_filter, me1, count, per, rows)
        else:
            outs = compress(x, g, me1, count, per, begin, rows, chunks[-1][0])
        pieces = [outs[0]]
        for s in range(1, count):
            pieces.append(cyclic(outs[s], "line", s))
        chunks.append(pieces)

    *phase, weights = phases(fm_rate[0], rcmc_weights, columns, splits)
    seam = jnp.concatenate([seam_width, seam_link])

    dop, images, heads, tails, energies = [], [], [], [], []
    begun = 0
    below = None
    blocks = []
    for n, group in enumerate(groups):
        after = [phase[0]] if n == 0 else energies[-1:]
        outs = doppler([chunks[c] for c in group], tw_forward, mat_forward, MARGIN if n == 0 else 0, after)
        dop.append(outs[0])
        blocks.append((starts[group[0]], outs[0].shape[2]))
        if n == 0:
            below = lax.ppermute(outs[1], "line", [(i, i - 1) for i in range(1, count)])
        held = sum(blocks[-1])
        while len(images) < len(splits):
            rows, factor = splits[len(images)], phase[len(images)]
            need = begun + rows + MARGIN
            if need > held and held < per:
                break
            parts = []
            for d, (b, n) in zip(dop, blocks):
                low, high = max(b, begun), min(b + n, -(-need // 8) * 8)
                if low < high:
                    parts.append((d, low - b, high - low))
            if need > per:
                parts.append((below, 0, MARGIN))
            i = len(images)
            image, head, tail, energy = focus_rows(
                parts, weights, rcmc_shift[0], factor, tw_inverse, mat_inverse, begun, rows,
                tails if i == len(splits) - 1 else [])
            images.append(image)
            heads.append(head)
            energies.append(energy)
            tails.append(tail)
            begun += rows
    earlier = lax.ppermute(tails[-1], "chip", [(j, j + 1) for j in range(chips - 1)])
    *mixed, energy = blend(heads, earlier, energies, seam)
    everyone = [energy] + [cyclic(energy, "line", s) for s in range(1, count)]
    return finish(images, mixed, everyone, float(RKEEP * length))


def solution(mesh):
    in_specs = (
        P("chip", None, "line", None),
        P(),
        P(),
        P("chip", "line"),
        P("chip", "line"),
        P("chip"),
        P("chip"),
    )
    out_specs = P("chip", None, "line", None)
    return jax.shard_map(strip, mesh=mesh, in_specs=in_specs, out_specs=out_specs, check_vma=False)
```

```python
import math

import jax
import jax.numpy as jnp
import numpy as np
from jax import lax
from jax.experimental import pallas as pl
from jax.experimental.pallas import tpu as pltpu
from jax.sharding import PartitionSpec as P


RKEEP = 384
TAPS = 8
MAXSHIFT = 12
LANES = 128
MARGIN = MAXSHIFT + TAPS - 1
HALO = 24

F32 = jnp.float32
ANY = pl.BlockSpec(memory_space=pl.ANY)
VMEM = pl.BlockSpec(memory_space=pltpu.VMEM)
BF16 = jnp.bfloat16


def split_np(table):
    high = table.astype(jnp.bfloat16)
    low = (table - high.astype(np.float64)).astype(jnp.bfloat16)
    return high, low


def root(length, index, sign):
    angle = sign * 2.0 * np.pi * (np.asarray(index) % length) / length
    return np.cos(angle), np.sin(angle)


def lane_matrix():
    index = np.arange(LANES)
    real, imag = root(LANES, np.outer(index, index), -1)
    return np.concatenate(split_np(np.block([[real, imag], [-imag, real]])), axis=0)


def lane_transform(value, mat_ref):
    high, low = split3(value)
    table = mat_ref[...]
    coarse, fine = table[:2 * LANES], table[2 * LANES:]
    return dot_nn(jnp.concatenate([high, low, high], axis=1), jnp.concatenate([coarse, coarse, fine], axis=0))


def column_twiddle(columns, length, sign, scale=1.0):
    real, imag = root(length, np.outer(np.arange(columns), np.arange(LANES)), sign)
    return (scale * np.stack([real, imag])).astype(np.float32)


def cmul_const(value, real, imag):
    vr, vi = value
    near = 1e-12
    if abs(imag) < near:
        if abs(real - 1.0) < near:
            return value
        if abs(real + 1.0) < near:
            return (-vr, -vi)
    if abs(real) < near:
        if imag > 0:
            return (-vi, vr)
        return (vi, -vr)
    if abs(abs(real) - abs(imag)) < near:
        mag = abs(real)
        sr, si = (1.0 if real > 0 else -1.0), (1.0 if imag > 0 else -1.0)
        if sr == si:
            return ((vr - vi) * (mag * sr), (vr + vi) * (mag * sr))
        return ((vr + vi) * (mag * sr), (vi - vr) * (mag * sr))
    return (vr * real - vi * imag, vr * imag + vi * real)


def cadd(a, b):
    return (a[0] + b[0], a[1] + b[1])


def csub(a, b):
    return (a[0] - b[0], a[1] - b[1])


def dft_list(values, sign):
    count = len(values)
    if count == 1:
        return values
    if count == 2:
        return [cadd(values[0], values[1]), csub(values[0], values[1])]
    if count == 4:
        even = [cadd(values[0], values[2]), csub(values[0], values[2])]
        odd = [cadd(values[1], values[3]), csub(values[1], values[3])]
        turn = cmul_const(odd[1], 0.0, float(sign))
        return [cadd(even[0], odd[0]), cadd(even[1], turn), csub(even[0], odd[0]), csub(even[1], turn)]
    even = dft_list(values[0::2], sign)
    odd = dft_list(values[1::2], sign)
    low, high = [], []
    for k in range(count // 2):
        real, imag = root(count, k, sign)
        turned = cmul_const(odd[k], float(real), float(imag))
        low.append(cadd(even[k], turned))
        high.append(csub(even[k], turned))
    return low + high


def split3(value):
    high = value.astype(BF16)
    low = (value - high.astype(F32)).astype(BF16)
    return high, low


def dot_nn(a, b):
    return lax.dot_general(a, b, (((1,), (0,)), ((), ())), preferred_element_type=F32)


def dot_nt(a, b):
    return lax.dot_general(a, b, (((1,), (1,)), ((), ())), preferred_element_type=F32)


def response_tables(length):
    columns = length // LANES
    group = LANES // columns
    index = np.arange(LANES)
    firsts = []
    for b in range(group):
        real, imag = root(LANES, np.outer(index, np.arange(columns) * group + b), -1)
        firsts.append(np.block([[real, -imag], [imag, real]]))
    first = np.concatenate(firsts, axis=1).astype(np.float32)
    tw = column_twiddle(columns, length, -1, 1.0 / length).reshape(2 * columns, LANES)
    real, imag = root(columns, np.outer(np.arange(columns), np.arange(columns)), -1)
    last = np.block([[real, -imag], [imag, real]]).astype(np.float32)
    table = np.zeros((2 * LANES + 2 * columns, max(2 * LANES, LANES + 2 * columns)), np.float32)
    table[:2 * LANES, :2 * LANES] = first
    table[2 * LANES:, :LANES] = tw
    table[2 * LANES:, LANES:LANES + 2 * columns] = last
    return table


def response(f_ref, table_ref, out_ref):
    columns = out_ref.shape[1]
    group = LANES // columns
    parts = []
    for c in range(2):
        parts.append(jnp.concatenate(
            [f_ref[c:c + 1, j * LANES:(j + 1) * LANES] for j in range(columns)], axis=0))
    blocks = []
    for b in range(group):
        sl = slice(columns * b, columns * (b + 1))
        blocks.append(jnp.concatenate([parts[0][:, sl], parts[1][:, sl]], axis=0))
    rhs = jnp.concatenate(blocks, axis=0)
    half = lax.dot_general(
        table_ref[:2 * LANES, :2 * LANES], rhs, (((1,), (0,)), ((), ())),
        precision=lax.Precision.HIGHEST, preferred_element_type=F32)
    re = half[:LANES].T
    im = half[LANES:].T
    twr = table_ref[2 * LANES:2 * LANES + columns, :LANES]
    twi = table_ref[2 * LANES + columns:2 * LANES + 2 * columns, :LANES]
    pair = jnp.concatenate([re * twr - im * twi, re * twi + im * twr], axis=0)
    full = lax.dot_general(
        table_ref[2 * LANES:, LANES:LANES + 2 * columns], pair, (((1,), (0,)), ((), ())),
        precision=lax.Precision.HIGHEST, preferred_element_type=F32)
    out_ref[0] = full[:columns]
    out_ref[1] = full[columns:]


def toeplitz(g_ref, table, count, per, start, rows, columns):
    base = [
        jnp.concatenate([jnp.broadcast_to(g_ref[c, j:j + 1, :], (8, LANES)) for j in range(columns)], axis=1)
        for c in range(2)
    ]
    base = [pltpu.roll(b, 0, 1, stride=1, stride_axis=0) for b in base]
    sub = lax.broadcasted_iota(jnp.int32, (8, LANES), 0)
    half = count * rows
    group = 16 if half % 16 == 0 else 8
    order = [per * d + start + r8 for d in range(count) for r8 in range(0, rows, 8)]
    for at in range(0, half, group):
        pieces = [[], []]
        for shift in order[at // 8:(at + group) // 8]:
            bins = (sub + shift).astype(F32)
            gain = 1.0 + 2.0 * bins / RKEEP
            gain = jnp.concatenate([gain] * columns, axis=1)
            for c in range(2):
                pieces[c].append(pltpu.roll(base[c], shift % (columns * LANES), 1) * gain)
        grh, grl = split3(jnp.concatenate(pieces[0], axis=0))
        gih, gil = split3(jnp.concatenate(pieces[1], axis=0))
        for n, (plain, crossed) in enumerate(((grh, -gih), (gih, grh), (grl, -gil), (gil, grl))):
            table[0, n * half + at:n * half + at + group, :] = plain
            table[1, n * half + at:n * half + at + group, :] = crossed


def scatter(me_ref, outs, turned):
    count = len(outs)
    for s in range(count):
        dest = lax.rem(me_ref[0] + s, count)
        outs[s][0] = turned[0, dest]
        outs[s][1] = turned[1, dest]


def turn(acc, turned, at):
    width = acc.shape[1] // 2
    both = acc[:, :width] + acc[:, width:]
    turned[:, :, :, pl.ds(at, acc.shape[0])] = both.T.reshape(turned.shape[:3] + (acc.shape[0],))


def compress_first(echoes, range_filter, me, count, per, rows, kept):
    lines, samples = echoes.shape[2], echoes.shape[3]
    columns = samples // LANES
    blocks = max(1, min(4, samples // 1024))
    kblk = samples // blocks
    width = 2 * count * rows
    mblk = min(512, lines)
    tables = response_tables(samples)

    def kernel(me_ref, x_hbm, f_hbm, t_hbm, *refs):
        outs, refs = refs[:count], refs[count:]
        g_ref, x_ref, keep_ref, f_ref, t_ref, table, acc, turned, sems = refs
        small = [pltpu.make_async_copy(f_hbm, f_ref, sems.at[2 * blocks]),
                 pltpu.make_async_copy(t_hbm, t_ref, sems.at[2 * blocks + 1])]
        large = []
        for k in range(blocks):
            for c in range(2):
                ks = slice(k * kblk, (k + 1) * kblk)
                large.append(pltpu.make_async_copy(
                    x_hbm.at[0, c, :, ks], x_ref.at[c, :, ks], sems.at[2 * k + c]))
        for copy in small + large:
            copy.start()
        for copy in small:
            copy.wait()
        response(f_ref, t_ref, g_ref)
        toeplitz(g_ref, table, count, per, 0, rows, columns)
        for k in range(blocks):
            ks = slice(k * kblk, (k + 1) * kblk)
            large[2 * k].wait()
            large[2 * k + 1].wait()

            def body(m, carry):
                at = pl.multiple_of(m * mblk, mblk)
                ms = pl.ds(at, mblk)
                part = dot_nt(x_ref[0, ms, ks], table[0, :, ks]) + dot_nt(x_ref[1, ms, ks], table[1, :, ks])
                if k > 0:
                    part = part + acc[ms, :]
                if k < blocks - 1:
                    acc[ms, :] = part
                else:
                    turn(part, turned, at)
                return carry

            lax.fori_loop(0, lines // mblk, body, 0)
        scatter(me_ref, outs, turned)
        keep_ref[...] = turned[:, kept]

    hbm = pl.BlockSpec(memory_space=pltpu.HBM)
    out = jax.ShapeDtypeStruct((2, rows, lines), F32)
    results = pl.pallas_call(
        kernel,
        in_specs=[pl.BlockSpec(memory_space=pltpu.SMEM), hbm, hbm, hbm],
        out_specs=[VMEM] * (count + 3),
        out_shape=[out] * count + [
            jax.ShapeDtypeStruct((2, columns, LANES), F32),
            jax.ShapeDtypeStruct((2, lines, samples), BF16), out],
        scratch_shapes=[
            pltpu.VMEM(range_filter.shape, F32),
            pltpu.VMEM(tables.shape, F32),
            pltpu.VMEM((2, 2 * width, samples), BF16),
            pltpu.VMEM((lines, 2 * width), F32),
            pltpu.VMEM((2, count, rows, lines), F32),
            pltpu.SemaphoreType.DMA((2 * blocks + 2,)),
        ],
        compiler_params=pltpu.CompilerParams(vmem_limit_bytes=(26 if rows * count <= 64 else 48) * 2**20),
        cost_estimate=pl.CostEstimate(
            flops=8 * lines * samples * 2 * width, bytes_accessed=4 * lines * samples, transcendentals=0),
        name="compress",
    )(me, echoes, range_filter, tables)
    return results[:count], *results[count:]


def compress(x, g, me, count, per, start, rows, kept, keep=None):
    lines, samples = x.shape[1], x.shape[2]
    columns = samples // LANES
    width = 2 * count * rows
    mblk = min(512, lines)
    again = start < MARGIN <= start + rows

    def kernel(me_ref, x_ref, g_ref, keep_ref, *refs):
        outs = refs[:count]
        table, turned = refs[-2:]
        toeplitz(g_ref, table, count, per, start, rows, columns)

        def body(m, carry):
            at = pl.multiple_of(m * mblk, mblk)
            ms = pl.ds(at, mblk)
            turn(dot_nt(x_ref[0, ms, :], table[0]) + dot_nt(x_ref[1, ms, :], table[1]), turned, at)
            return carry

        lax.fori_loop(0, lines // mblk, body, 0)
        scatter(me_ref, outs, turned)
        if again:
            for c in range(2):
                refs[count][c * MARGIN:c * MARGIN + start, :] = keep_ref[c]
                refs[count][c * MARGIN + start:(c + 1) * MARGIN, :] = turned[c, kept, :MARGIN - start, :]

    return pl.pallas_call(
        kernel,
        in_specs=[pl.BlockSpec(memory_space=pltpu.SMEM), VMEM, VMEM, VMEM if again else ANY],
        out_specs=[VMEM] * (count + again),
        out_shape=[jax.ShapeDtypeStruct((2, rows, lines), F32)] * count
        + [jax.ShapeDtypeStruct((2 * MARGIN, lines), F32)] * again,
        scratch_shapes=[
            pltpu.VMEM((2, 2 * width, samples), BF16),
            pltpu.VMEM((2, count, rows, lines), F32),
        ],
        compiler_params=pltpu.CompilerParams(vmem_limit_bytes=(9 + rows * count // 10) * 2**20),
        cost_estimate=pl.CostEstimate(
            flops=8 * lines * samples * 2 * width, bytes_accessed=4 * lines * samples, transcendentals=0),
        name="compress",
    )(me, x, g, keep)


def doppler(chunks, flat, tw, matrix, lead, after):
    count = len(chunks[0])
    lines = chunks[0][0].shape[2]
    sizes = [pieces[0].shape[1] for pieces in chunks]
    rows = sum(sizes)
    own = lines // LANES
    columns = own * count
    number = count * len(chunks) + len(flat)
    total = rows + (HALO if flat else 0)

    def kernel(*refs):
        tw_ref, mat_ref = refs[number:number + 2]
        outs, scratch = refs[number + 2 + len(after):-1], refs[-1]
        out_ref = outs[0]

        def group(ins, load, r8, place):
            inner = [[None] * own for _ in range(count)]
            for p in range(own):
                ls = slice(p * LANES, (p + 1) * LANES)
                spread = dft_list([(load(ref, 0, r8, ls), load(ref, 1, r8, ls)) for ref in ins], 1)
                for k0 in range(count):
                    real, imag = root(columns, p * k0, -1)
                    inner[k0][p] = cmul_const(spread[k0], float(real), float(imag))
            for k0 in range(count):
                for k1, (vr, vi) in enumerate(dft_list(inner[k0], -1)):
                    k = k0 + count * k1
                    tr = tw_ref[0, k:k + 1, :]
                    ti = tw_ref[1, k:k + 1, :]
                    scratch[place(k), :LANES] = vr * tr - vi * ti
                    scratch[place(k), LANES:] = vr * ti + vi * tr

        begun = 0
        for n, size in enumerate(sizes):
            ins = refs[n * count:(n + 1) * count]

            def load(ref, c, r8, ls):
                return ref[c, pl.ds(r8, 8), ls]

            def body(i, carry, ins=ins, begun=begun):
                r8 = pl.multiple_of(i * 8, 8)
                group(ins, load, r8, lambda k: pl.ds(pl.multiple_of(k * total + begun + r8, 8), 8))
                return carry

            lax.fori_loop(0, size // 8, body, 0)
            begun += size
        if flat:
            def load_flat(ref, c, r8, ls):
                return ref[c * MARGIN + r8:c * MARGIN + r8 + 8, ls]

            for r8 in (*range(0, MARGIN - 8, 8), MARGIN - 8):
                group(refs[number - count:number], load_flat, r8,
                      lambda k: slice(k * total + rows + r8, k * total + rows + r8 + 8))
        out = lane_transform(scratch[...], mat_ref)
        for c in range(2):
            part = out[:, c * LANES:(c + 1) * LANES].reshape(columns, total, LANES)
            out_ref[c] = part[:, :rows, :]
            if flat:
                for k in range(columns):
                    at = (c * columns + k) * MARGIN
                    outs[-1][at:at + MARGIN, :] = part[k, rows:rows + MARGIN, :]
        if lead:
            for c in range(2):
                for k in range(columns):
                    at = (c * columns + k) * lead
                    outs[1][at:at + lead, :] = out_ref[c, k, :lead, :]

    return pl.pallas_call(
        kernel,
        in_specs=[VMEM] * (number + 2) + [ANY] * len(after),
        out_shape=[jax.ShapeDtypeStruct((2, columns, rows, LANES), F32)]
        + [jax.ShapeDtypeStruct((2 * columns * MARGIN, LANES), F32)] * ((lead > 0) + (len(flat) > 0)),
        compiler_params=pltpu.CompilerParams(vmem_limit_bytes=(4 + total // 5) * 2**20),
        scratch_shapes=[pltpu.VMEM((columns * total, 2 * LANES), F32)],
        cost_estimate=pl.CostEstimate(
            flops=2 * columns * rows * 256 * 768, bytes_accessed=16 * columns * rows * LANES, transcendentals=0),
        name="doppler",
    )(*[piece for pieces in chunks for piece in pieces], *flat, tw, matrix, *after)


def turn_pair(turns):
    folds = jnp.floor(2.0 * turns + 0.5)
    rest = turns - 0.5 * folds
    sign = 1.0 - 2.0 * (folds - 2.0 * jnp.floor(0.5 * folds))
    z = rest * rest
    cos_c = [(-1) ** j * (2 * math.pi) ** (2 * j) / math.factorial(2 * j) for j in range(7)]
    sin_c = [(-1) ** j * (2 * math.pi) ** (2 * j + 1) / math.factorial(2 * j + 1) for j in range(7)]
    c = cos_c[-1] * z + cos_c[-2]
    s = sin_c[-1] * z + sin_c[-2]
    for j in range(4, -1, -1):
        c = c * z + cos_c[j]
        s = s * z + sin_c[j]
    return c * sign, s * (rest * sign)


def phases(fm, weights, columns, splits):
    pick = np.zeros((LANES, LANES), np.float32)
    width = LANES // columns
    for b in range(width):
        for p in range(columns):
            pick[b * columns + p, width * p + b] = 1.0
    per = fm.shape[0]
    length = columns * LANES
    coarse = 2048
    together = 4

    def kernel(fm_ref, w_ref, pick_ref, *outs):
        outs, w_out = outs[:-1], outs[-1]

        @pl.when(pl.program_id(0) == 0)
        def _():
            rows_in = []
            for t in range(TAPS):
                tap = jnp.concatenate(
                    [w_ref[t:t + 1, p * LANES:(p + 1) * LANES] for p in range(columns)], axis=0).T
                rows_in.append(jnp.concatenate(
                    [tap[b * columns:(b + 1) * columns, :] for b in range(width)], axis=1))
            w_out[...] = lax.dot_general(
                jnp.concatenate(rows_in, axis=0), pick_ref[...], (((1,), (0,)), ((), ())),
                precision=lax.Precision.HIGHEST, preferred_element_type=F32)

        for i in range(together):
            k = pl.program_id(0) * together + i
            lane = lax.broadcasted_iota(jnp.int32, (1, LANES), 1)
            index = k + columns * lane
            index = jnp.where(index >= length // 2, index - length, index)
            square = index * index
            upper = (square // coarse).astype(F32)
            lower = (square % coarse).astype(F32)
            scale = 1.0 / (2.0 * length * length)
            first = 0
            for out, rows in zip(outs, splits):
                rate = fm_ref[first:first + rows, :]
                whole = jnp.floor(rate)
                part = rate - whole
                turns = whole * (upper * (coarse * scale))
                turns = turns - jnp.floor(turns)
                turns = turns + whole * (lower * scale) + part * (square.astype(F32) * scale)
                c, s = turn_pair(turns)
                out[0, i] = c
                out[1, i] = -s
                first += rows

    return pl.pallas_call(
        kernel,
        grid=(columns // together,),
        in_specs=[pl.BlockSpec(a, lambda k: (0, 0)) for a in ((per, LANES), weights.shape, pick.shape)],
        out_specs=[pl.BlockSpec((2, together, rows, LANES), lambda k: (0, k, 0, 0)) for rows in splits]
        + [pl.BlockSpec((TAPS * columns, LANES), lambda k: (0, 0))],
        out_shape=[jax.ShapeDtypeStruct((2, columns, rows, LANES), F32) for rows in splits]
        + [jax.ShapeDtypeStruct((TAPS * columns, LANES), F32)],
        cost_estimate=pl.CostEstimate(
            flops=60 * columns * per * LANES, bytes_accessed=8 * columns * per * LANES, transcendentals=0),
        compiler_params=pltpu.CompilerParams(vmem_limit_bytes=8 * 2**20),
        name="phases",
    )(jnp.broadcast_to(fm[:, None], (per, LANES)), weights, pick)


def focus_rows(parts, weights, shift, me, mid, phase, tw, matrix, first, rows, earlier):
    columns = phase.shape[1]
    total = sum(take for a, _, take in parts if len(a.shape) == 4) + MARGIN
    reach = -(-(rows + MAXSHIFT) // 8) * 8
    pitch_d = max(total, reach + 8)
    pitch_d += 1 - pitch_d % 2
    pitch_u = reach + 1
    pitch_m = rows + 1

    def kernel(shift_ref, me_ref, *refs):
        ins = refs[:len(parts)]
        middle = me_ref[0] == mid
        w_ref, ph_ref, tw_ref, mat_ref = refs[len(parts):len(parts) + 4]
        before = refs[len(parts) + 4:len(parts) + 4 + len(earlier)]
        out_ref, head_ref, tail_ref, en_ref, dop, sums, moved, scratch = refs[len(parts) + 4 + len(earlier):]
        base = 0
        for ref in before:
            tail_ref[:, base:base + ref.shape[1], :] = ref[...]
            base += ref.shape[1]

        def combine(k, carry):
            taps = [w_ref[pl.ds(t * columns + k, 1), :] for t in range(TAPS)]
            for c in range(2):
                at = (c * columns + k) * pitch_d
                filled = 0
                for ref, (a, begin, take) in zip(ins, parts):
                    if len(a.shape) == 4:
                        dop[pl.ds(at + filled, take), :] = ref[c, k, begin:begin + take, :]
                        filled += take
                flat = [ref[pl.ds((c * columns + k) * MARGIN, MARGIN), :]
                        for ref, (a, _, _) in zip(ins, parts) if len(a.shape) == 2]
                if flat:
                    piece = jnp.where(middle, flat[1], flat[0]) if len(flat) > 1 else flat[0]
                    dop[pl.ds(at + filled, MARGIN), :] = piece
                    filled += MARGIN
                if filled < reach + 8:
                    dop[pl.ds(at + filled, reach + 8 - filled), :] = jnp.zeros((reach + 8 - filled, LANES), F32)
                to = (c * columns + k) * pitch_u
                for r8 in range(0, reach, 8):
                    value = taps[0] * dop[pl.ds(at + r8, 8), :]
                    for t in range(1, TAPS):
                        value = value + taps[t] * dop[pl.ds(at + r8 + t, 8), :]
                    sums[pl.ds(to + r8, 8), :] = value
            return carry

        lax.fori_loop(0, columns, combine, 0)

        def move(r, carry):
            source = r + shift_ref[first + r]
            for c in range(2):
                for k8 in range(0, columns, 8):
                    lead = c * columns + k8
                    moved[pl.ds(lead * pitch_m + r, 8, stride=pitch_m), :] = (
                        sums[pl.ds(lead * pitch_u + source, 8, stride=pitch_u), :])
            return carry

        lax.fori_loop(0, rows, move, 0)

        for k in range(columns):
            at = slice(k * rows, (k + 1) * rows)
            vr = moved[k * pitch_m:k * pitch_m + rows, :]
            vi = moved[(columns + k) * pitch_m:(columns + k) * pitch_m + rows, :]
            pr, pi = ph_ref[0, k], ph_ref[1, k]
            scratch[at, :LANES] = vr * pi + vi * pr
            scratch[at, LANES:] = vr * pr - vi * pi
        scratch[...] = lane_transform(scratch[...], mat_ref)

        def transform(i, total_energy):
            r8 = pl.multiple_of(i * 8, 8)
            rs = pl.ds(r8, 8)
            values = []
            for k in range(columns):
                at = pl.ds(pl.multiple_of(k * rows + r8, 8), 8)
                vi, vr = scratch[at, :LANES], scratch[at, LANES:]
                tr, ti = tw_ref[0, k:k + 1, :], tw_ref[1, k:k + 1, :]
                values.append((vr * tr - vi * ti, vr * ti + vi * tr))
            for j, pair in enumerate(dft_list(values, 1)):
                ls = slice(j * LANES, (j + 1) * LANES)
                for c in range(2):
                    if j == 0:
                        head_ref[c, rs, :] = pair[c]
                    else:
                        out_ref[c, rs, ls] = pair[c]
                        total_energy = total_energy + pair[c] * pair[c]
                    if j == columns - 1:
                        tail_ref[c, pl.ds(pl.multiple_of(base + r8, 8), 8), :] = pair[c]
            return total_energy

        total_energy = lax.fori_loop(0, rows // 8, transform, jnp.zeros((8, LANES), F32))
        en_ref[...] = total_energy

    return pl.pallas_call(
        kernel,
        in_specs=[pl.BlockSpec(memory_space=pltpu.SMEM)] * 2 + [VMEM] * (len(parts) + 4 + len(earlier)),
        out_shape=[
            jax.ShapeDtypeStruct((2, rows, columns * LANES), F32),
            jax.ShapeDtypeStruct((2, rows, LANES), F32),
            jax.ShapeDtypeStruct((2, rows + sum(a.shape[1] for a in earlier), LANES), F32),
            jax.ShapeDtypeStruct((8, LANES), F32),
        ],
        scratch_shapes=[
            pltpu.VMEM((-(-2 * columns * pitch_d // 8) * 8 + 8, LANES), F32),
            pltpu.VMEM((-(-2 * columns * pitch_u // 8) * 8 + 8, LANES), F32),
            pltpu.VMEM((-(-2 * columns * pitch_m // 8) * 8 + 8, LANES), F32),
            pltpu.VMEM((columns * rows, 2 * LANES), F32),
        ],
        compiler_params=pltpu.CompilerParams(vmem_limit_bytes=(16 if rows < 32 else 26 if rows < 48 else 32) * 2**20),
        cost_estimate=pl.CostEstimate(
            flops=2 * columns * rows * 256 * 768, bytes_accessed=32 * columns * rows * LANES, transcendentals=0),
        name="focus",
    )(shift, me, *[a for a, _, _ in parts], weights, phase, tw, matrix, *earlier)


def blend(heads, earlier, energies, seam):
    number = len(heads)

    def kernel(seam_ref, *refs):
        head_refs, tail_ref, energy_refs = refs[:number], refs[number], refs[number + 1:-number - 1]
        outs, total_ref = refs[-number - 1:-1], refs[-1]
        width, linked = seam_ref[0], seam_ref[1]
        total = energy_refs[0][...]
        for ref in energy_refs[1:]:
            total = total + ref[...]
        first = 0
        for head, out in zip(head_refs, outs):
            rows = head.shape[1]
            for c in range(2):
                now = head[c]
                offsets = lax.broadcasted_iota(jnp.int32, now.shape, 1)
                ramp = (offsets.astype(F32) + 0.5) / width.astype(F32)
                inside = (offsets < width) & (linked == 1)
                before = pltpu.roll(tail_ref[c, first:first + rows, :], width, 1)
                mixed = jnp.where(inside, (1.0 - ramp) * before + ramp * now, now)
                out[c] = mixed
                power = mixed * mixed
                for r8 in range(0, rows, 8):
                    total = total + power[r8:r8 + 8]
            first += rows
        total_ref[...] = total

    return pl.pallas_call(
        kernel,
        in_specs=[pl.BlockSpec(memory_space=pltpu.SMEM)] + [VMEM] * (number + 1 + len(energies)),
        out_shape=[jax.ShapeDtypeStruct(h.shape, F32) for h in heads] + [jax.ShapeDtypeStruct((8, LANES), F32)],
        compiler_params=pltpu.CompilerParams(vmem_limit_bytes=4 * 2**20),
        name="blend",
    )(seam, *heads, earlier, *energies)


def finish(images, heads, energies, pixels):
    number, count = len(images), len(energies)
    total_rows = sum(a.shape[1] for a in images)
    length = images[0].shape[2]

    def kernel(*refs):
        image_refs, head_refs = refs[:number], refs[number:2 * number]
        energy_refs, out_ref = refs[2 * number:-1], refs[-1]
        total = energy_refs[0][...]
        for ref in energy_refs[1:]:
            total = total + ref[...]
        energy = jnp.sum(jnp.sum(total, axis=0, keepdims=True), axis=1, keepdims=True)
        scale = lax.rsqrt(energy / pixels + 1e-06)
        for c in range(2):
            for j in range(length // LANES):
                ls = slice(j * LANES, (j + 1) * LANES)
                rows = [ref[c] if j == 0 else ref[c, :, ls] for ref in (head_refs if j == 0 else image_refs)]
                out_ref[0, c, :, ls] = (jnp.concatenate(rows, axis=0) * scale).astype(BF16)

    return pl.pallas_call(
        kernel,
        in_specs=[VMEM] * (2 * number + count),
        out_shape=jax.ShapeDtypeStruct((1, 2, total_rows, length), BF16),
        compiler_params=pltpu.CompilerParams(vmem_limit_bytes=12 * 2**20),
        name="finish",
    )(*images, *heads, *energies)


def cyclic(value, axis, steps):
    count = lax.axis_size(axis)
    return lax.ppermute(value, axis, [(i, (i + steps) % count) for i in range(count)])


def plan(per):
    if per == 96:
        return [16, 16, 32, 32], [[0, 1], [2], [3]], [40, 56]
    return [per], [[0]], [per]


def strip(echoes, range_filter, rcmc_weights, fm_rate, rcmc_shift, seam_width, seam_link):
    count = lax.axis_size("line")
    chips = lax.axis_size("chip")
    me = lax.axis_index("line").astype(jnp.int32)
    lines = echoes.shape[2]
    length = lines * count
    columns = length // LANES
    per = fm_rate.shape[1]

    turn = root(count, np.outer(np.arange(count), np.arange(columns)), -1)
    base = column_twiddle(columns, length, -1).astype(np.float64)
    tw_all = np.stack([
        turn[0][:, :, None] * base[0] - turn[1][:, :, None] * base[1],
        turn[0][:, :, None] * base[1] + turn[1][:, :, None] * base[0]], axis=1).astype(np.float32)
    tw_forward = lax.dynamic_index_in_dim(jnp.asarray(tw_all), me, 0, keepdims=False)
    tw_inverse = column_twiddle(columns, length, 1, 1.0 / length)
    matrix = lane_matrix()

    me1 = me.reshape(1)
    sizes, groups, splits = plan(per)
    starts = [sum(sizes[:c]) for c in range(len(sizes))]
    mid = count // 2 - 1
    raw, chunks = [], []
    dop, blocks, below = [], [], []

    def azimuth(flat, after):
        n = len(dop)
        lead = MARGIN if n == 0 else 0
        outs = doppler([chunks[c] for c in groups[n]], flat, tw_forward, matrix, lead, after)
        dop.append(outs[0])
        blocks.append((starts[groups[n][0]], outs[0].shape[2]))
        if lead:
            alone = len(groups) == 1
            below.append(lax.ppermute(
                outs[1], "line", [(i, i - 1) for i in range(1, count) if alone or i != mid + 1]))
        below.extend(outs[1 + (lead > 0):])
        return outs[-1]

    for c, (begin, rows) in enumerate(zip(starts, sizes)):
        if c == 1:
            last = keep
        elif c > 0:
            last = chunks[-1][0]
        if c == 0:
            outs, g, x, keep = compress_first(echoes, range_filter, me1, count, per, rows, mid + 1)
        else:
            outs = compress(x, g, me1, count, per, begin, rows, mid + 1, last)
        pieces = [outs[0]]
        for s in range(1, count):
            pieces.append(cyclic(outs[s], "line", s))
        chunks.append(pieces)
        if len(outs) > count:
            raw = [outs[count]]
            for s in range(1, count):
                raw.append(lax.ppermute(outs[count], "line", [((mid - s) % count, mid)]))

    azimuth([], [])
    *phase, weights = phases(fm_rate[0], rcmc_weights, columns, splits)
    seam = jnp.concatenate([seam_width, seam_link])

    images, heads, tails, energies = [], [], [], []
    begun = 0
    while len(images) < len(splits):
        if len(dop) < len(groups):
            azimuth(raw if len(dop) == 1 else [], [phase[0]] if len(dop) < 2 else energies[-1:])
        held = sum(blocks[-1])
        while len(images) < len(splits):
            i = len(images)
            rows, factor = splits[i], phase[i]
            need = begun + rows + MARGIN
            if need > held and held < per:
                break
            parts = []
            for d, (b, n) in zip(dop, blocks):
                low, high = max(b, begun), min(b + n, -(-need // 8) * 8)
                if low < high:
                    parts.append((d, low - b, high - low))
            if need > per:
                parts += [(a, 0, MARGIN) for a in below]
            image, head, tail, energy = focus_rows(
                parts, weights, rcmc_shift[0], me1, mid, factor, tw_inverse, matrix, begun, rows,
                tails if i == len(splits) - 1 else [])
            images.append(image)
            heads.append(head)
            energies.append(energy)
            tails.append(tail)
            begun += rows
    earlier = lax.ppermute(tails[-1], "chip", [(j, j + 1) for j in range(chips - 1)])
    *mixed, energy = blend(heads, earlier, energies, seam)
    everyone = [energy] + [cyclic(energy, "line", s) for s in range(1, count)]
    return finish(images, mixed, everyone, float(RKEEP * length))


def solution(mesh):
    in_specs = (
        P("chip", None, "line", None),
        P(),
        P(),
        P("chip", "line"),
        P("chip", "line"),
        P("chip"),
        P("chip"),
    )
    out_specs = P("chip", None, "line", None)
    return jax.shard_map(strip, mesh=mesh, in_specs=in_specs, out_specs=out_specs, check_vma=False)
```

```python
import math

import jax
import jax.numpy as jnp
import numpy as np
from jax import lax
from jax.experimental import pallas as pl
from jax.experimental.pallas import tpu as pltpu
from jax.sharding import PartitionSpec as P


RKEEP = 384
TAPS = 8
MAXSHIFT = 12
LANES = 128
MARGIN = MAXSHIFT + TAPS - 1
HALO = 24

F32 = jnp.float32
ANY = pl.BlockSpec(memory_space=pl.ANY)
VMEM = pl.BlockSpec(memory_space=pltpu.VMEM)
BF16 = jnp.bfloat16


def split_np(table):
    high = table.astype(jnp.bfloat16)
    low = (table - high.astype(np.float64)).astype(jnp.bfloat16)
    return high, low


def root(length, index, sign):
    angle = sign * 2.0 * np.pi * (np.asarray(index) % length) / length
    return np.cos(angle), np.sin(angle)


def lane_matrix():
    index = np.arange(LANES)
    real, imag = root(LANES, np.outer(index, index), -1)
    return np.concatenate(split_np(np.block([[real, imag], [-imag, real]])), axis=0)


def lane_transform(value, mat_ref):
    high, low = split3(value)
    table = mat_ref[...]
    coarse, fine = table[:2 * LANES], table[2 * LANES:]
    return dot_nn(jnp.concatenate([high, low, high], axis=1), jnp.concatenate([coarse, coarse, fine], axis=0))


def column_twiddle(columns, length, sign, scale=1.0):
    real, imag = root(length, np.outer(np.arange(columns), np.arange(LANES)), sign)
    return (scale * np.stack([real, imag])).astype(np.float32)


def cmul_const(value, real, imag):
    vr, vi = value
    near = 1e-12
    if abs(imag) < near:
        if abs(real - 1.0) < near:
            return value
        if abs(real + 1.0) < near:
            return (-vr, -vi)
    if abs(real) < near:
        if imag > 0:
            return (-vi, vr)
        return (vi, -vr)
    if abs(abs(real) - abs(imag)) < near:
        mag = abs(real)
        sr, si = (1.0 if real > 0 else -1.0), (1.0 if imag > 0 else -1.0)
        if sr == si:
            return ((vr - vi) * (mag * sr), (vr + vi) * (mag * sr))
        return ((vr + vi) * (mag * sr), (vi - vr) * (mag * sr))
    return (vr * real - vi * imag, vr * imag + vi * real)


def cadd(a, b):
    return (a[0] + b[0], a[1] + b[1])


def csub(a, b):
    return (a[0] - b[0], a[1] - b[1])


def dft_list(values, sign):
    count = len(values)
    if count == 1:
        return values
    if count == 2:
        return [cadd(values[0], values[1]), csub(values[0], values[1])]
    if count == 4:
        even = [cadd(values[0], values[2]), csub(values[0], values[2])]
        odd = [cadd(values[1], values[3]), csub(values[1], values[3])]
        turn = cmul_const(odd[1], 0.0, float(sign))
        return [cadd(even[0], odd[0]), cadd(even[1], turn), csub(even[0], odd[0]), csub(even[1], turn)]
    even = dft_list(values[0::2], sign)
    odd = dft_list(values[1::2], sign)
    low, high = [], []
    for k in range(count // 2):
        real, imag = root(count, k, sign)
        turned = cmul_const(odd[k], float(real), float(imag))
        low.append(cadd(even[k], turned))
        high.append(csub(even[k], turned))
    return low + high


def split3(value):
    high = value.astype(BF16)
    low = (value - high.astype(F32)).astype(BF16)
    return high, low


def dot_nn(a, b):
    return lax.dot_general(a, b, (((1,), (0,)), ((), ())), preferred_element_type=F32)


def dot_nt(a, b):
    return lax.dot_general(a, b, (((1,), (1,)), ((), ())), preferred_element_type=F32)


def response_tables(length):
    columns = length // LANES
    group = LANES // columns
    index = np.arange(LANES)
    firsts = []
    for b in range(group):
        real, imag = root(LANES, np.outer(index, np.arange(columns) * group + b), -1)
        firsts.append(np.block([[real, -imag], [imag, real]]))
    first = np.concatenate(firsts, axis=1).astype(np.float32)
    tw = column_twiddle(columns, length, -1, 1.0 / length).reshape(2 * columns, LANES)
    real, imag = root(columns, np.outer(np.arange(columns), np.arange(columns)), -1)
    last = np.block([[real, -imag], [imag, real]]).astype(np.float32)
    table = np.zeros((2 * LANES + 2 * columns, max(2 * LANES, LANES + 2 * columns)), np.float32)
    table[:2 * LANES, :2 * LANES] = first
    table[2 * LANES:, :LANES] = tw
    table[2 * LANES:, LANES:LANES + 2 * columns] = last
    return table


def response(f_ref, table_ref, out_ref):
    columns = out_ref.shape[1]
    group = LANES // columns
    parts = []
    for c in range(2):
        parts.append(jnp.concatenate(
            [f_ref[c:c + 1, j * LANES:(j + 1) * LANES] for j in range(columns)], axis=0))
    blocks = []
    for b in range(group):
        sl = slice(columns * b, columns * (b + 1))
        blocks.append(jnp.concatenate([parts[0][:, sl], parts[1][:, sl]], axis=0))
    rhs = jnp.concatenate(blocks, axis=0)
    half = lax.dot_general(
        table_ref[:2 * LANES, :2 * LANES], rhs, (((1,), (0,)), ((), ())),
        precision=lax.Precision.HIGHEST, preferred_element_type=F32)
    re = half[:LANES].T
    im = half[LANES:].T
    twr = table_ref[2 * LANES:2 * LANES + columns, :LANES]
    twi = table_ref[2 * LANES + columns:2 * LANES + 2 * columns, :LANES]
    pair = jnp.concatenate([re * twr - im * twi, re * twi + im * twr], axis=0)
    full = lax.dot_general(
        table_ref[2 * LANES:, LANES:LANES + 2 * columns], pair, (((1,), (0,)), ((), ())),
        precision=lax.Precision.HIGHEST, preferred_element_type=F32)
    out_ref[0] = full[:columns]
    out_ref[1] = full[columns:]


def toeplitz(g_ref, table, count, per, start, rows, columns):
    base = [
        jnp.concatenate([jnp.broadcast_to(g_ref[c, j:j + 1, :], (8, LANES)) for j in range(columns)], axis=1)
        for c in range(2)
    ]
    base = [pltpu.roll(b, 0, 1, stride=1, stride_axis=0) for b in base]
    sub = lax.broadcasted_iota(jnp.int32, (8, LANES), 0)
    half = count * rows
    group = 16 if half % 16 == 0 else 8
    order = [per * d + start + r8 for d in range(count) for r8 in range(0, rows, 8)]
    for at in range(0, half, group):
        pieces = [[], []]
        for shift in order[at // 8:(at + group) // 8]:
            bins = (sub + shift).astype(F32)
            gain = 1.0 + 2.0 * bins / RKEEP
            gain = jnp.concatenate([gain] * columns, axis=1)
            for c in range(2):
                pieces[c].append(pltpu.roll(base[c], shift % (columns * LANES), 1) * gain)
        grh, grl = split3(jnp.concatenate(pieces[0], axis=0))
        gih, gil = split3(jnp.concatenate(pieces[1], axis=0))
        for n, (plain, crossed) in enumerate(((grh, -gih), (gih, grh), (grl, -gil), (gil, grl))):
            table[0, n * half + at:n * half + at + group, :] = plain
            table[1, n * half + at:n * half + at + group, :] = crossed


def scatter(me_ref, outs, turned):
    count = len(outs)
    for s in range(count):
        dest = lax.rem(me_ref[0] + s, count)
        outs[s][0] = turned[0, dest]
        outs[s][1] = turned[1, dest]


def turn(acc, turned, at):
    width = acc.shape[1] // 2
    both = acc[:, :width] + acc[:, width:]
    turned[:, :, :, pl.ds(at, acc.shape[0])] = both.T.reshape(turned.shape[:3] + (acc.shape[0],))


def compress_first(echoes, range_filter, me, count, per, rows, kept):
    lines, samples = echoes.shape[2], echoes.shape[3]
    columns = samples // LANES
    blocks = max(1, min(4, samples // 1024))
    kblk = samples // blocks
    width = 2 * count * rows
    mblk = min(512, lines)
    tables = response_tables(samples)

    def kernel(me_ref, x_hbm, f_hbm, t_hbm, *refs):
        outs, refs = refs[:count], refs[count:]
        g_ref, x_ref, keep_ref, f_ref, t_ref, table, acc, turned, sems = refs
        small = [pltpu.make_async_copy(f_hbm, f_ref, sems.at[2 * blocks]),
                 pltpu.make_async_copy(t_hbm, t_ref, sems.at[2 * blocks + 1])]
        large = []
        for k in range(blocks):
            for c in range(2):
                ks = slice(k * kblk, (k + 1) * kblk)
                large.append(pltpu.make_async_copy(
                    x_hbm.at[0, c, :, ks], x_ref.at[c, :, ks], sems.at[2 * k + c]))
        for copy in small + large:
            copy.start()
        for copy in small:
            copy.wait()
        response(f_ref, t_ref, g_ref)
        toeplitz(g_ref, table, count, per, 0, rows, columns)
        for k in range(blocks):
            ks = slice(k * kblk, (k + 1) * kblk)
            large[2 * k].wait()
            large[2 * k + 1].wait()

            def body(m, carry):
                at = pl.multiple_of(m * mblk, mblk)
                ms = pl.ds(at, mblk)
                part = dot_nt(x_ref[0, ms, ks], table[0, :, ks]) + dot_nt(x_ref[1, ms, ks], table[1, :, ks])
                if k > 0:
                    part = part + acc[ms, :]
                if k < blocks - 1:
                    acc[ms, :] = part
                else:
                    turn(part, turned, at)
                return carry

            lax.fori_loop(0, lines // mblk, body, 0)
        scatter(me_ref, outs, turned)
        keep_ref[...] = turned[:, kept]

    hbm = pl.BlockSpec(memory_space=pltpu.HBM)
    out = jax.ShapeDtypeStruct((2, rows, lines), F32)
    results = pl.pallas_call(
        kernel,
        in_specs=[pl.BlockSpec(memory_space=pltpu.SMEM), hbm, hbm, hbm],
        out_specs=[VMEM] * (count + 3),
        out_shape=[out] * count + [
            jax.ShapeDtypeStruct((2, columns, LANES), F32),
            jax.ShapeDtypeStruct((2, lines, samples), BF16), out],
        scratch_shapes=[
            pltpu.VMEM(range_filter.shape, F32),
            pltpu.VMEM(tables.shape, F32),
            pltpu.VMEM((2, 2 * width, samples), BF16),
            pltpu.VMEM((lines, 2 * width), F32),
            pltpu.VMEM((2, count, rows, lines), F32),
            pltpu.SemaphoreType.DMA((2 * blocks + 2,)),
        ],
        compiler_params=pltpu.CompilerParams(vmem_limit_bytes=(26 if rows * count <= 64 else 48) * 2**20),
        cost_estimate=pl.CostEstimate(
            flops=8 * lines * samples * 2 * width, bytes_accessed=4 * lines * samples, transcendentals=0),
        name="compress",
    )(me, echoes, range_filter, tables)
    return results[:count], *results[count:]


def compress(x, g, me, count, per, start, rows, kept, keep=None):
    lines, samples = x.shape[1], x.shape[2]
    columns = samples // LANES
    width = 2 * count * rows
    mblk = min(1024 if rows <= 16 else 512, lines)
    again = start < MARGIN <= start + rows

    def kernel(me_ref, x_ref, g_ref, keep_ref, *refs):
        outs = refs[:count]
        table, turned = refs[-2:]
        toeplitz(g_ref, table, count, per, start, rows, columns)

        def body(m, carry):
            at = pl.multiple_of(m * mblk, mblk)
            ms = pl.ds(at, mblk)
            turn(dot_nt(x_ref[0, ms, :], table[0]) + dot_nt(x_ref[1, ms, :], table[1]), turned, at)
            return carry

        lax.fori_loop(0, lines // mblk, body, 0)
        scatter(me_ref, outs, turned)
        if again:
            for c in range(2):
                refs[count][c * MARGIN:c * MARGIN + start, :] = keep_ref[c]
                refs[count][c * MARGIN + start:(c + 1) * MARGIN, :] = turned[c, kept, :MARGIN - start, :]

    return pl.pallas_call(
        kernel,
        in_specs=[pl.BlockSpec(memory_space=pltpu.SMEM), VMEM, VMEM, VMEM if again else ANY],
        out_specs=[VMEM] * (count + again),
        out_shape=[jax.ShapeDtypeStruct((2, rows, lines), F32)] * count
        + [jax.ShapeDtypeStruct((2 * MARGIN, lines), F32)] * again,
        scratch_shapes=[
            pltpu.VMEM((2, 2 * width, samples), BF16),
            pltpu.VMEM((2, count, rows, lines), F32),
        ],
        compiler_params=pltpu.CompilerParams(vmem_limit_bytes=(9 + rows * count // 10) * 2**20),
        cost_estimate=pl.CostEstimate(
            flops=8 * lines * samples * 2 * width, bytes_accessed=4 * lines * samples, transcendentals=0),
        name="compress",
    )(me, x, g, keep)


def doppler(chunks, flat, me, tw, matrix, lead, after):
    count = len(chunks[0])
    lines = chunks[0][0].shape[2]
    sizes = [pieces[0].shape[1] for pieces in chunks]
    rows = sum(sizes)
    own = lines // LANES
    columns = own * count
    number = count * len(chunks) + len(flat)
    total = rows + (HALO if flat else 0)

    def kernel(me_ref, *refs):
        tw_ref, mat_ref = refs[number:number + 2]
        own_tw = tw_ref.at[me_ref[0]]
        outs, scratch = refs[number + 2 + len(after):-1], refs[-1]
        out_ref = outs[0]

        def group(ins, load, r8, place):
            inner = [[None] * own for _ in range(count)]
            for p in range(own):
                ls = slice(p * LANES, (p + 1) * LANES)
                spread = dft_list([(load(ref, 0, r8, ls), load(ref, 1, r8, ls)) for ref in ins], 1)
                for k0 in range(count):
                    real, imag = root(columns, p * k0, -1)
                    inner[k0][p] = cmul_const(spread[k0], float(real), float(imag))
            for k0 in range(count):
                for k1, (vr, vi) in enumerate(dft_list(inner[k0], -1)):
                    k = k0 + count * k1
                    tr = own_tw[0, k:k + 1, :]
                    ti = own_tw[1, k:k + 1, :]
                    scratch[place(k), :LANES] = vr * tr - vi * ti
                    scratch[place(k), LANES:] = vr * ti + vi * tr

        begun = 0
        for n, size in enumerate(sizes):
            ins = refs[n * count:(n + 1) * count]

            def load(ref, c, r8, ls):
                return ref[c, pl.ds(r8, 8), ls]

            def body(i, carry, ins=ins, begun=begun):
                r8 = pl.multiple_of(i * 8, 8)
                group(ins, load, r8, lambda k: pl.ds(pl.multiple_of(k * total + begun + r8, 8), 8))
                return carry

            lax.fori_loop(0, size // 8, body, 0)
            begun += size
        if flat:
            def load_flat(ref, c, r8, ls):
                return ref[c * MARGIN + r8:c * MARGIN + r8 + 8, ls]

            for r8 in (*range(0, MARGIN - 8, 8), MARGIN - 8):
                group(refs[number - count:number], load_flat, r8,
                      lambda k: slice(k * total + rows + r8, k * total + rows + r8 + 8))
        out = lane_transform(scratch[...], mat_ref)
        for c in range(2):
            part = out[:, c * LANES:(c + 1) * LANES].reshape(columns, total, LANES)
            out_ref[c] = part[:, :rows, :]
            if flat:
                for k in range(columns):
                    at = (c * columns + k) * MARGIN
                    outs[-1][at:at + MARGIN, :] = part[k, rows:rows + MARGIN, :]
        if lead:
            for c in range(2):
                for k in range(columns):
                    at = (c * columns + k) * lead
                    outs[1][at:at + lead, :] = out_ref[c, k, :lead, :]

    return pl.pallas_call(
        kernel,
        in_specs=[pl.BlockSpec(memory_space=pltpu.SMEM)] + [VMEM] * (number + 2) + [ANY] * len(after),
        out_shape=[jax.ShapeDtypeStruct((2, columns, rows, LANES), F32)]
        + [jax.ShapeDtypeStruct((2 * columns * MARGIN, LANES), F32)] * ((lead > 0) + (len(flat) > 0)),
        compiler_params=pltpu.CompilerParams(vmem_limit_bytes=(4 + total // 5) * 2**20),
        scratch_shapes=[pltpu.VMEM((columns * total, 2 * LANES), F32)],
        cost_estimate=pl.CostEstimate(
            flops=2 * columns * rows * 256 * 768, bytes_accessed=16 * columns * rows * LANES, transcendentals=0),
        name="doppler",
    )(me, *[piece for pieces in chunks for piece in pieces], *flat, tw, matrix, *after)


def turn_pair(turns):
    folds = jnp.floor(2.0 * turns + 0.5)
    rest = turns - 0.5 * folds
    sign = 1.0 - 2.0 * (folds - 2.0 * jnp.floor(0.5 * folds))
    z = rest * rest
    cos_c = [(-1) ** j * (2 * math.pi) ** (2 * j) / math.factorial(2 * j) for j in range(7)]
    sin_c = [(-1) ** j * (2 * math.pi) ** (2 * j + 1) / math.factorial(2 * j + 1) for j in range(7)]
    c = cos_c[-1] * z + cos_c[-2]
    s = sin_c[-1] * z + sin_c[-2]
    for j in range(4, -1, -1):
        c = c * z + cos_c[j]
        s = s * z + sin_c[j]
    return c * sign, s * (rest * sign)


def phases(fm, weights, columns, splits):
    pick = np.zeros((LANES, LANES), np.float32)
    width = LANES // columns
    for b in range(width):
        for p in range(columns):
            pick[b * columns + p, width * p + b] = 1.0
    per = fm.shape[0]
    length = columns * LANES
    coarse = 2048
    together = 4

    def kernel(fm_ref, w_ref, pick_ref, *outs):
        outs, w_out = outs[:-1], outs[-1]

        @pl.when(pl.program_id(0) == 0)
        def _():
            rows_in = []
            for t in range(TAPS):
                tap = jnp.concatenate(
                    [w_ref[t:t + 1, p * LANES:(p + 1) * LANES] for p in range(columns)], axis=0).T
                rows_in.append(jnp.concatenate(
                    [tap[b * columns:(b + 1) * columns, :] for b in range(width)], axis=1))
            w_out[...] = lax.dot_general(
                jnp.concatenate(rows_in, axis=0), pick_ref[...], (((1,), (0,)), ((), ())),
                precision=lax.Precision.HIGHEST, preferred_element_type=F32)

        for i in range(together):
            k = pl.program_id(0) * together + i
            lane = lax.broadcasted_iota(jnp.int32, (1, LANES), 1)
            index = k + columns * lane
            index = jnp.where(index >= length // 2, index - length, index)
            square = index * index
            upper = (square // coarse).astype(F32)
            lower = (square % coarse).astype(F32)
            scale = 1.0 / (2.0 * length * length)
            first = 0
            for out, rows in zip(outs, splits):
                rate = fm_ref[first:first + rows, :]
                whole = jnp.floor(rate)
                part = rate - whole
                turns = whole * (upper * (coarse * scale))
                turns = turns - jnp.floor(turns)
                turns = turns + whole * (lower * scale) + part * (square.astype(F32) * scale)
                c, s = turn_pair(turns)
                out[0, i] = c
                out[1, i] = -s
                first += rows

    return pl.pallas_call(
        kernel,
        grid=(columns // together,),
        in_specs=[pl.BlockSpec(a, lambda k: (0, 0)) for a in ((per, LANES), weights.shape, pick.shape)],
        out_specs=[pl.BlockSpec((2, together, rows, LANES), lambda k: (0, k, 0, 0)) for rows in splits]
        + [pl.BlockSpec((TAPS * columns, LANES), lambda k: (0, 0))],
        out_shape=[jax.ShapeDtypeStruct((2, columns, rows, LANES), F32) for rows in splits]
        + [jax.ShapeDtypeStruct((TAPS * columns, LANES), F32)],
        cost_estimate=pl.CostEstimate(
            flops=60 * columns * per * LANES, bytes_accessed=8 * columns * per * LANES, transcendentals=0),
        compiler_params=pltpu.CompilerParams(vmem_limit_bytes=8 * 2**20),
        name="phases",
    )(jnp.broadcast_to(fm[:, None], (per, LANES)), weights, pick)


def focus_rows(parts, weights, shift, me, mid, phase, tw, matrix, first, rows, earlier):
    columns = phase.shape[1]
    total = sum(take for a, _, take in parts if len(a.shape) == 4) + MARGIN
    reach = -(-(rows + MAXSHIFT) // 8) * 8
    pitch_d = max(total, reach + 8)
    pitch_d += 1 - pitch_d % 2
    pitch_u = reach + 1
    pitch_m = rows + 1

    def kernel(shift_ref, me_ref, *refs):
        ins = refs[:len(parts)]
        middle = me_ref[0] == mid
        w_ref, ph_ref, tw_ref, mat_ref = refs[len(parts):len(parts) + 4]
        before = refs[len(parts) + 4:len(parts) + 4 + len(earlier)]
        out_ref, head_ref, tail_ref, en_ref, dop, sums, moved, scratch = refs[len(parts) + 4 + len(earlier):]
        base = 0
        for ref in before:
            tail_ref[:, base:base + ref.shape[1], :] = ref[...]
            base += ref.shape[1]

        def combine(k, carry):
            taps = [w_ref[pl.ds(t * columns + k, 1), :] for t in range(TAPS)]
            for c in range(2):
                at = (c * columns + k) * pitch_d
                filled = 0
                for ref, (a, begin, take) in zip(ins, parts):
                    if len(a.shape) == 4:
                        dop[pl.ds(at + filled, take), :] = ref[c, k, begin:begin + take, :]
                        filled += take
                flat = [ref[pl.ds((c * columns + k) * MARGIN, MARGIN), :]
                        for ref, (a, _, _) in zip(ins, parts) if len(a.shape) == 2]
                if flat:
                    piece = jnp.where(middle, flat[1], flat[0]) if len(flat) > 1 else flat[0]
                    dop[pl.ds(at + filled, MARGIN), :] = piece
                    filled += MARGIN
                if filled < reach + 8:
                    dop[pl.ds(at + filled, reach + 8 - filled), :] = jnp.zeros((reach + 8 - filled, LANES), F32)
                to = (c * columns + k) * pitch_u
                for r8 in range(0, reach, 8):
                    value = taps[0] * dop[pl.ds(at + r8, 8), :]
                    for t in range(1, TAPS):
                        value = value + taps[t] * dop[pl.ds(at + r8 + t, 8), :]
                    sums[pl.ds(to + r8, 8), :] = value
            return carry

        lax.fori_loop(0, columns, combine, 0)

        def move(r, carry):
            source = r + shift_ref[first + r]
            for c in range(2):
                for k8 in range(0, columns, 8):
                    lead = c * columns + k8
                    moved[pl.ds(lead * pitch_m + r, 8, stride=pitch_m), :] = (
                        sums[pl.ds(lead * pitch_u + source, 8, stride=pitch_u), :])
            return carry

        lax.fori_loop(0, rows, move, 0)

        for k in range(columns):
            at = slice(k * rows, (k + 1) * rows)
            vr = moved[k * pitch_m:k * pitch_m + rows, :]
            vi = moved[(columns + k) * pitch_m:(columns + k) * pitch_m + rows, :]
            pr, pi = ph_ref[0, k], ph_ref[1, k]
            scratch[at, :LANES] = vr * pi + vi * pr
            scratch[at, LANES:] = vr * pr - vi * pi
        scratch[...] = lane_transform(scratch[...], mat_ref)

        def transform(i, total_energy):
            r8 = pl.multiple_of(i * 8, 8)
            rs = pl.ds(r8, 8)
            values = []
            for k in range(columns):
                at = pl.ds(pl.multiple_of(k * rows + r8, 8), 8)
                vi, vr = scratch[at, :LANES], scratch[at, LANES:]
                tr, ti = tw_ref[0, k:k + 1, :], tw_ref[1, k:k + 1, :]
                values.append((vr * tr - vi * ti, vr * ti + vi * tr))
            for j, pair in enumerate(dft_list(values, 1)):
                ls = slice(j * LANES, (j + 1) * LANES)
                for c in range(2):
                    if j == 0:
                        head_ref[c, rs, :] = pair[c]
                    else:
                        out_ref[c, rs, ls] = pair[c]
                        total_energy = total_energy + pair[c] * pair[c]
                    if j == columns - 1:
                        tail_ref[c, pl.ds(pl.multiple_of(base + r8, 8), 8), :] = pair[c]
            return total_energy

        total_energy = lax.fori_loop(0, rows // 8, transform, jnp.zeros((8, LANES), F32))
        en_ref[...] = total_energy

    return pl.pallas_call(
        kernel,
        in_specs=[pl.BlockSpec(memory_space=pltpu.SMEM)] * 2 + [VMEM] * (len(parts) + 4 + len(earlier)),
        out_shape=[
            jax.ShapeDtypeStruct((2, rows, columns * LANES), F32),
            jax.ShapeDtypeStruct((2, rows, LANES), F32),
            jax.ShapeDtypeStruct((2, rows + sum(a.shape[1] for a in earlier), LANES), F32),
            jax.ShapeDtypeStruct((8, LANES), F32),
        ],
        scratch_shapes=[
            pltpu.VMEM((-(-2 * columns * pitch_d // 8) * 8 + 8, LANES), F32),
            pltpu.VMEM((-(-2 * columns * pitch_u // 8) * 8 + 8, LANES), F32),
            pltpu.VMEM((-(-2 * columns * pitch_m // 8) * 8 + 8, LANES), F32),
            pltpu.VMEM((columns * rows, 2 * LANES), F32),
        ],
        compiler_params=pltpu.CompilerParams(vmem_limit_bytes=(16 if rows < 32 else 26 if rows < 48 else 32) * 2**20),
        cost_estimate=pl.CostEstimate(
            flops=2 * columns * rows * 256 * 768, bytes_accessed=32 * columns * rows * LANES, transcendentals=0),
        name="focus",
    )(shift, me, *[a for a, _, _ in parts], weights, phase, tw, matrix, *earlier)


def blend(heads, earlier, energies, seam):
    number = len(heads)

    def kernel(seam_ref, *refs):
        head_refs, tail_ref, energy_refs = refs[:number], refs[number], refs[number + 1:-number - 1]
        outs, total_ref = refs[-number - 1:-1], refs[-1]
        width, linked = seam_ref[0], seam_ref[1]
        total = energy_refs[0][...]
        for ref in energy_refs[1:]:
            total = total + ref[...]
        first = 0
        for head, out in zip(head_refs, outs):
            rows = head.shape[1]
            for c in range(2):
                now = head[c]
                offsets = lax.broadcasted_iota(jnp.int32, now.shape, 1)
                ramp = (offsets.astype(F32) + 0.5) / width.astype(F32)
                inside = (offsets < width) & (linked == 1)
                before = pltpu.roll(tail_ref[c, first:first + rows, :], width, 1)
                mixed = jnp.where(inside, (1.0 - ramp) * before + ramp * now, now)
                out[c] = mixed
                power = mixed * mixed
                for r8 in range(0, rows, 8):
                    total = total + power[r8:r8 + 8]
            first += rows
        total_ref[...] = total

    return pl.pallas_call(
        kernel,
        in_specs=[pl.BlockSpec(memory_space=pltpu.SMEM)] + [VMEM] * (number + 1 + len(energies)),
        out_shape=[jax.ShapeDtypeStruct(h.shape, F32) for h in heads] + [jax.ShapeDtypeStruct((8, LANES), F32)],
        compiler_params=pltpu.CompilerParams(vmem_limit_bytes=4 * 2**20),
        name="blend",
    )(seam, *heads, earlier, *energies)


def finish(images, heads, energies, pixels):
    number, count = len(images), len(energies)
    total_rows = sum(a.shape[1] for a in images)
    length = images[0].shape[2]

    def kernel(*refs):
        image_refs, head_refs = refs[:number], refs[number:2 * number]
        energy_refs, out_ref = refs[2 * number:-1], refs[-1]
        total = energy_refs[0][...]
        for ref in energy_refs[1:]:
            total = total + ref[...]
        energy = jnp.sum(jnp.sum(total, axis=0, keepdims=True), axis=1, keepdims=True)
        scale = lax.rsqrt(energy / pixels + 1e-06)
        for c in range(2):
            for j in range(length // LANES):
                ls = slice(j * LANES, (j + 1) * LANES)
                rows = [ref[c] if j == 0 else ref[c, :, ls] for ref in (head_refs if j == 0 else image_refs)]
                out_ref[0, c, :, ls] = (jnp.concatenate(rows, axis=0) * scale).astype(BF16)

    return pl.pallas_call(
        kernel,
        in_specs=[VMEM] * (2 * number + count),
        out_shape=jax.ShapeDtypeStruct((1, 2, total_rows, length), BF16),
        compiler_params=pltpu.CompilerParams(vmem_limit_bytes=12 * 2**20),
        name="finish",
    )(*images, *heads, *energies)


def cyclic(value, axis, steps):
    count = lax.axis_size(axis)
    return lax.ppermute(value, axis, [(i, (i + steps) % count) for i in range(count)])


def plan(per):
    if per == 96:
        return [16, 16, 32, 32], [[0, 1], [2], [3]], [40, 32, 24]
    return [per], [[0]], [per]


def strip(echoes, range_filter, rcmc_weights, fm_rate, rcmc_shift, seam_width, seam_link):
    count = lax.axis_size("line")
    chips = lax.axis_size("chip")
    me = lax.axis_index("line").astype(jnp.int32)
    lines = echoes.shape[2]
    length = lines * count
    columns = length // LANES
    per = fm_rate.shape[1]

    turn = root(count, np.outer(np.arange(count), np.arange(columns)), -1)
    base = column_twiddle(columns, length, -1).astype(np.float64)
    tw_all = np.stack([
        turn[0][:, :, None] * base[0] - turn[1][:, :, None] * base[1],
        turn[0][:, :, None] * base[1] + turn[1][:, :, None] * base[0]], axis=1).astype(np.float32)
    tw_inverse = column_twiddle(columns, length, 1, 1.0 / length)
    matrix = lane_matrix()

    me1 = me.reshape(1)
    sizes, groups, splits = plan(per)
    starts = [sum(sizes[:c]) for c in range(len(sizes))]
    mid = count // 2 - 1
    raw, chunks = [], []
    dop, blocks, below = [], [], []

    def azimuth(flat, after):
        n = len(dop)
        lead = MARGIN if n == 0 else 0
        outs = doppler([chunks[c] for c in groups[n]], flat, me1, tw_all, matrix, lead, after)
        dop.append(outs[0])
        blocks.append((starts[groups[n][0]], outs[0].shape[2]))
        if lead:
            alone = len(groups) == 1
            below.append(lax.ppermute(
                outs[1], "line", [(i, i - 1) for i in range(1, count) if alone or i != mid + 1]))
        below.extend(outs[1 + (lead > 0):])
        return outs[-1]

    for c, (begin, rows) in enumerate(zip(starts, sizes)):
        if c == 1:
            last = keep
        elif c > 0:
            last = chunks[-1][0]
        if c == 0:
            outs, g, x, keep = compress_first(echoes, range_filter, me1, count, per, rows, mid + 1)
        else:
            outs = compress(x, g, me1, count, per, begin, rows, mid + 1, last)
        pieces = [outs[0]]
        for s in range(1, count):
            pieces.append(cyclic(outs[s], "line", s))
        chunks.append(pieces)
        if len(outs) > count:
            raw = [outs[count]]
            for s in range(1, count):
                raw.append(lax.ppermute(outs[count], "line", [((mid - s) % count, mid)]))

    azimuth([], [])
    *phase, weights = phases(fm_rate[0], rcmc_weights, columns, splits)
    seam = jnp.concatenate([seam_width, seam_link])

    images, heads, tails, energies = [], [], [], []
    begun = 0
    while len(images) < len(splits):
        if len(dop) < len(groups):
            azimuth(raw if len(dop) == 1 else [], [phase[0]] if len(dop) < 2 else energies[-1:])
        held = sum(blocks[-1])
        while len(images) < len(splits):
            i = len(images)
            rows, factor = splits[i], phase[i]
            need = begun + rows + MARGIN
            if need > held and held < per:
                break
            parts = []
            for d, (b, n) in zip(dop, blocks):
                low, high = max(b, begun), min(b + n, -(-need // 8) * 8)
                if low < high:
                    parts.append((d, low - b, high - low))
            if need > per:
                parts += [(a, 0, MARGIN) for a in below]
            image, head, tail, energy = focus_rows(
                parts, weights, rcmc_shift[0], me1, mid, factor, tw_inverse, matrix, begun, rows,
                tails if i == len(splits) - 1 else [])
            images.append(image)
            heads.append(head)
            energies.append(energy)
            tails.append(tail)
            begun += rows
    earlier = lax.ppermute(tails[-1], "chip", [(j, j + 1) for j in range(chips - 1)])
    *mixed, energy = blend(heads, earlier, energies, seam)
    everyone = [energy] + [cyclic(energy, "line", s) for s in range(1, count)]
    return finish(images, mixed, everyone, float(RKEEP * length))


def solution(mesh):
    in_specs = (
        P("chip", None, "line", None),
        P(),
        P(),
        P("chip", "line"),
        P("chip", "line"),
        P("chip"),
        P("chip"),
    )
    out_specs = P("chip", None, "line", None)
    return jax.shard_map(strip, mesh=mesh, in_specs=in_specs, out_specs=out_specs, check_vma=False)
```
